256 devices in a mesh: gx: 8 (over y_hi, x), gy: 8 (over z), gz: 4 (over y_lo, core).
Axes of the slice: x: 4, y: 4 (y_hi: 2, y_lo: 2; y = y_hi * 2 + y_lo), z: 8, core: 2. Of those that a mesh axis runs over, the one named last changes fastest.
Arguments:
- populations: float32 [39, 64, 192, 512], P(None, 'gx', 'gy', 'gz'), may hold values from 0.5 to 1.5
- relax: float32 [64, 192, 512], P('gx', 'gy', 'gz'), may hold values from 0.6 to 1.9
Outputs:
- advanced: float32 [39, 64, 192, 512], P(None, 'gx', 'gy', 'gz')
The draws below stay inside these ranges and needn't reach their ends.
All inputs are finite; a program needn't handle non-finite values.
Results may differ from the reference program's by a relative error of at most 0.0001.
Values sent between devices are 32-bit elements; how exact they have to be, the bound alone decides.
A program may use at most 128 MiB of HBM per device.

```python
import math
import jax
import jax.numpy as jnp

Q = 39
STEPS = 1
NX = 64
NY = 192
NZ = 512


def steps_of(stream_key, shape, cuts, least, high):
    level, own = 1.0, jax.random.fold_in(stream_key, 6)
    for position, blocks in cuts:
        heights = jnp.exp(jax.random.uniform(jax.random.fold_in(own, position), (blocks,), jnp.float32, least / len(cuts), high / len(cuts)))
        level = level * jnp.repeat(heights, shape[position] // blocks).reshape([-1 if axis == position else 1 for axis in range(len(shape))])
    return level


def setup_inputs(seed: int = 0) -> dict:
    splits = jax.random.split(jax.random.key(seed), 3)
    return {
        "populations": jnp.clip(0.5 + 1.0 * jax.random.uniform(splits[0], (Q, NX, NY, NZ), jnp.float32) ** steps_of(splits[0], (Q, NX, NY, NZ), ((1, 8), (2, 8), (3, 4)), -0.2, 0.2), 0.5, 1.5),
        "relax": jnp.clip(jnp.exp(math.log(1.9) - 1.1526795 * jax.random.uniform(splits[1], (NX, NY, NZ), jnp.float32) ** steps_of(splits[1], (NX, NY, NZ), ((0, 8), (1, 8), (2, 4)), -0.2, 0.2)), 0.6, 1.9),
    }


def lattice():
    speeds = [(0, 0, 0)]
    weights = [1.0 / 12.0]
    for axis in range(3):
        for sign in (1, -1):
            vector = [0, 0, 0]
            vector[axis] = sign
            speeds.append(tuple(vector))
            weights.append(1.0 / 12.0)
    for first in (1, -1):
        for second in (1, -1):
            for third in (1, -1):
                speeds.append((first, second, third))
                weights.append(1.0 / 27.0)
    for axis in range(3):
        for sign in (2, -2):
            vector = [0, 0, 0]
            vector[axis] = sign
            speeds.append(tuple(vector))
            weights.append(2.0 / 135.0)
    for couple in ((0, 1), (0, 2), (1, 2)):
        for first in (2, -2):
            for second in (2, -2):
                vector = [0, 0, 0]
                vector[couple[0]] = first
                vector[couple[1]] = second
                speeds.append(tuple(vector))
                weights.append(1.0 / 432.0)
    for axis in range(3):
        for sign in (3, -3):
            vector = [0, 0, 0]
            vector[axis] = sign
            speeds.append(tuple(vector))
            weights.append(1.0 / 1620.0)
    return speeds, weights


def collide(popul, rate):
    speeds, weights = lattice()
    acoustic_wave_rate = 2.0 / 3.0
    inverse = 1.0 / (acoustic_wave_rate ** 0.5)
    zeroth_moment_rho = sum(weights[member] * popul[member] for member in range(39))
    flux = [sum(weights[member] * speeds[member][axis] * popul[member] for member in range(39) if speeds[member][axis] != 0) for axis in range(3)]
    thermal_heat_content = sum(weights[member] * float(sum(value * value for value in speeds[member])) * popul[member] for member in range(1, 39))
    velocity = [part / zeroth_moment_rho for part in flux]
    flow_norm_square = velocity[0] * velocity[0] + velocity[1] * velocity[1] + velocity[2] * velocity[2]
    site_kinetic_heat = (thermal_heat_content / zeroth_moment_rho - flow_norm_square) / (3.0 * acoustic_wave_rate)
    scaled = [part * inverse for part in velocity]
    scaled_square = flow_norm_square / acoustic_wave_rate
    excess_quantity = site_kinetic_heat - 1.0
    results = []
    for member in range(39):
        vector = speeds[member]
        aligned = sum(vector[axis] * inverse * scaled[axis] for axis in range(3) if vector[axis] != 0) if member > 0 else jnp.zeros_like(zeroth_moment_rho)
        speed_square = float(sum(value * value for value in vector)) / acoustic_wave_rate
        aligned_square = aligned * aligned
        hermite = (1.0 + aligned
                   + 0.5 * (aligned_square - scaled_square + excess_quantity * (speed_square - 3.0))
                   + aligned * (aligned_square - 3.0 * scaled_square + 3.0 * excess_quantity * (speed_square - 5.0)) / 6.0
                   + (aligned_square * aligned_square - 6.0 * aligned_square * scaled_square + 3.0 * scaled_square * scaled_square
                      + 6.0 * excess_quantity * (aligned_square * (speed_square - 7.0) + scaled_square * (5.0 - speed_square))
                      + 3.0 * excess_quantity * excess_quantity * (speed_square * speed_square - 10.0 * speed_square + 15.0)) / 24.0)
        maxwellian_target = zeroth_moment_rho * hermite
        results.append(popul[member] - rate * (popul[member] - maxwellian_target))
    return jnp.stack(results)


def reference(populations, relax):
    speeds, weights = lattice()
    state = populations
    for number in range(STEPS):
        post = collide(state, relax)
        state = jnp.stack([jnp.roll(post[member], speeds[member], axis=(0, 1, 2)) for member in range(39)])
    return state
```

```python
import functools

import jax
import jax.numpy as jnp
from jax import lax
from jax.experimental import pallas as pl
from jax.experimental.pallas import tpu as pltpu
from jax.sharding import PartitionSpec as P

MESH = pl.DeviceIdType.MESH
F32 = jnp.float32


def lattice():
    speeds = [(0, 0, 0)]
    weights = [1.0 / 12.0]
    for axis in range(3):
        for sign in (1, -1):
            vector = [0, 0, 0]
            vector[axis] = sign
            speeds.append(tuple(vector))
            weights.append(1.0 / 12.0)
    for first in (1, -1):
        for second in (1, -1):
            for third in (1, -1):
                speeds.append((first, second, third))
                weights.append(1.0 / 27.0)
    for axis in range(3):
        for sign in (2, -2):
            vector = [0, 0, 0]
            vector[axis] = sign
            speeds.append(tuple(vector))
            weights.append(2.0 / 135.0)
    for couple in ((0, 1), (0, 2), (1, 2)):
        for first in (2, -2):
            for second in (2, -2):
                vector = [0, 0, 0]
                vector[couple[0]] = first
                vector[couple[1]] = second
                speeds.append(tuple(vector))
                weights.append(1.0 / 432.0)
    for axis in range(3):
        for sign in (3, -3):
            vector = [0, 0, 0]
            vector[axis] = sign
            speeds.append(tuple(vector))
            weights.append(1.0 / 1620.0)
    return speeds, weights


SPEEDS, WEIGHTS = lattice()
Q = 39
INDEX = {vector: member for member, vector in enumerate(SPEEDS)}
ROWS = 32


def slots(axis, sign):
    table, offset = {}, 0
    for member in range(Q):
        speed = SPEEDS[member][axis] * sign
        if speed > 0:
            table[member] = offset
            offset += speed
    return table


XS = {sign: slots(0, sign) for sign in (1, -1)}
YS = {sign: slots(1, sign) for sign in (1, -1)}
ZS = {sign: slots(2, sign) for sign in (1, -1)}
EARLY = {sign: [m for m in XS[sign] if SPEEDS[m][2] == 0 and abs(SPEEDS[m][0]) < 3] for sign in (1, -1)}
THIRD = {sign: [m for m in XS[sign] if abs(SPEEDS[m][0]) == 3] for sign in (1, -1)}
LATE = {sign: [m for m in XS[sign] if SPEEDS[m][2] != 0] for sign in (1, -1)}
CORNERS = [(1, 1), (1, -1), (-1, 1), (-1, -1)]
SHELLS = {0.0: "0", 1.0: "1", 3.0: "c", 4.0: "2", 8.0: "e", 9.0: "3"}


def square(member):
    return float(sum(value * value for value in SPEEDS[member]))


def final_row(member):
    return 8 if SPEEDS[member][1] < 0 else 0


def corner_rows(sx, sy):
    rows = []
    for member in range(Q):
        cx, cy = SPEEDS[member][0] * sx, SPEEDS[member][1] * sy
        if cx > 0 and cy > 0:
            rows += [(member, layer, row) for layer in range(cx) for row in range(cy)]
    return rows


def leaving_row(member, row, ny):
    cy = SPEEDS[member][1]
    return ny + row if cy > 0 else 8 + cy + row


def entering_row(member, row, ny):
    cy = SPEEDS[member][1]
    return row if cy > 0 else 8 + ny + cy + row


def strided(ref, member, row):
    count, layers, rows, lanes = ref.shape
    return ref.reshape(count * layers * rows, lanes), pl.ds(member * layers * rows + row, layers, stride=rows)


def read_rows(ref, member, row):
    flat, where = strided(ref, member, row)
    return flat[where, :]


def write_rows(ref, member, row, value):
    flat, where = strided(ref, member, row)
    flat[where, :] = value


def collide(load, rate, store):
    weight = {shell: WEIGHTS[m] for m in range(Q) for shell in [SHELLS[square(m)]]}
    total = {}
    odd = {}
    for member in range(Q):
        vector = SPEEDS[member]
        shell = SHELLS[square(member)]
        opposite = INDEX[tuple(-value for value in vector)]
        if member == opposite:
            total[shell] = load(member)
        elif member < opposite:
            one, other = load(member), load(opposite)
            both = one + other
            total[shell] = total[shell] + both if shell in total else both
            odd[member] = one - other
    density = sum(weight[shell] * total[shell] for shell in total)
    energy = sum(weight[SHELLS[v]] * v * total[SHELLS[v]] for v in (1.0, 3.0, 4.0, 8.0, 9.0))
    inverse = 1.0 / density
    drift = []
    for axis in range(3):
        parts = {}
        for member, value in odd.items():
            speed = SPEEDS[member][axis]
            if speed == 0:
                continue
            key = (SHELLS[square(member)], abs(speed))
            if key in parts:
                parts[key] = parts[key] + value if speed > 0 else parts[key] - value
            else:
                parts[key] = value if speed > 0 else -value
        flux = sum((weight[shell] * speed * 1.5) * value for (shell, speed), value in parts.items())
        drift.append(flux * inverse)
    w = drift
    ww = [value * value for value in w]
    norm = (ww[0] + ww[1] + ww[2]) * (4.0 / 9.0)
    t = (energy * inverse - norm) * 0.5 - 1.0
    b = 1.5 * norm
    scale = rate * density
    keep = 1.0 - rate
    tb = t * b
    t2 = t * t
    p0 = scale * (1.0 - 0.5 * b + 0.125 * b * b - 1.5 * t + 1.25 * tb + 1.875 * t2)
    p1 = scale * (0.5 * t - 0.25 * tb - 1.25 * t2)
    p2 = scale * (0.125 * t2)
    st = scale * t
    b0 = scale * (0.5 - 0.25 * b) - 1.75 * st
    c0 = scale * (1.0 - 0.5 * b) - 2.5 * st
    quart = {k: (k**4 / 24.0) * scale for k in (1, 2, 3)}
    cubic = {k: (k**3 / 6.0) * scale for k in (1, 2, 3)}
    reach = {"1": 1, "c": 1, "2": 2, "e": 2, "3": 3}
    coefficients = {}
    for value, shell in SHELLS.items():
        s = 1.5 * value
        even = p0 + s * p1 + (s * s) * p2 if s else p0
        if s:
            k = reach[shell]
            coefficients[shell] = (
                even,
                (k * k) * b0 + (k * k * s * 0.25) * st,
                k * c0 + (k * s * 0.5) * st,
                quart[k],
                cubic[k],
            )
        else:
            coefficients[shell] = even
    for member in range(Q):
        vector = SPEEDS[member]
        shell = SHELLS[square(member)]
        opposite = INDEX[tuple(-value for value in vector)]
        if member == opposite:
            store(member, keep * load(member) + coefficients[shell])
        elif member < opposite:
            k = reach[shell]
            q, q2 = None, None
            axes = [axis for axis in range(3) if vector[axis] != 0]
            if len(axes) == 1:
                q, q2 = w[axes[0]], ww[axes[0]]
            else:
                q = w[axes[0]]
                for axis in axes[1:]:
                    q = q + w[axis] if vector[axis] > 0 else q - w[axis]
                q2 = q * q
            e0, e2, o1, e4, o3 = coefficients[shell]
            even = e0 + q2 * (e2 + q2 * e4)
            uneven = q * (o1 + q2 * o3)
            store(member, keep * load(member) + (even + uneven))
            store(opposite, keep * load(opposite) + (even - uneven))


def exchange_kernel(
    sizes, g_hbm, r_hbm, p_ref, up_ref, down_ref,
    g, rate, zraw, zsend, zrecv, ysend, yrecv, dsend, drecv,
    load_sem, z_sem, y_sem, d_sem, x_sem,
):
    nx, ny, nz = sizes
    pairs = nx // 2
    blocks = ny // 8
    order = [pairs - 1, 0] + [pair for pair in range(pairs - 2, 0, -1)]
    around = {}
    for axis in ("gx", "gy", "gz"):
        me, count = lax.axis_index(axis), lax.axis_size(axis)
        around[axis] = {1: lax.rem(me + 1, count), -1: lax.rem(me + count - 1, count)}

    loads = {}
    for turn, pair in enumerate(order):
        layers = pl.ds(2 * pair, 2)
        loads[pair] = [
            pltpu.make_async_copy(g_hbm.at[:, layers], g.at[:, layers], load_sem.at[turn]),
        ]
    rate_load = pltpu.make_async_copy(r_hbm, rate, load_sem.at[pairs])
    rate_load.start()
    for pair in order:
        for copy in loads[pair]:
            copy.start()

    barrier = pltpu.get_barrier_semaphore()
    friends = [{axis: around[axis][sign]} for axis in ("gx", "gy", "gz") for sign in (1, -1)]
    friends += [{"gx": around["gx"][sx], "gy": around["gy"][sy]} for sx, sy in CORNERS]
    for friend in friends:
        pl.semaphore_signal(barrier, inc=1, device_id=friend, device_id_type=MESH)

    lane = lax.broadcasted_iota(jnp.int32, (8, nz), 1)
    pack_masks = {offset: lane >= offset for offset in sorted(set(ZS[1].values())) if offset}

    def row_of(member, x, block):
        vector = SPEEDS[member]
        return pl.ds(final_row(member) + vector[1] + 8 * block, 8)

    def collide_block(x, block):
        packed = {1: None, -1: None}

        def load(member):
            return g[member, x, pl.ds(8 * block, 8), :]

        def store(member, value):
            cz = SPEEDS[member][2]
            if cz != 0:
                p_ref[member, x, row_of(member, x, block), :] = pltpu.roll(value, cz % nz, 1)
                sign = 1 if cz > 0 else -1
                place = ZS[sign][member]
                shift = (place + max(cz, 0)) % nz
                pieces.setdefault(sign, {})[place] = pltpu.roll(value, shift, 1) if shift else value
            else:
                p_ref[member, x, row_of(member, x, block), :] = value

        pieces = {}
        collide(load, rate[x, pl.ds(8 * block, 8), :], store)
        for index, sign in enumerate((1, -1)):
            packed = None
            for place in sorted(pieces[sign]):
                packed = pieces[sign][place] if packed is None else jnp.where(pack_masks[place], pieces[sign][place], packed)
            zraw[index, x, block] = packed

    def collide_pair(pair):
        def body(half, carry):
            for block in range(blocks):
                collide_block(2 * pair + half, block)
            return carry

        lax.fori_loop(0, 2, body, 0)

    def z_copy(pair, index):
        sign = (1, -1)[index]
        return pltpu.make_async_remote_copy(
            zsend.at[index, pair], zrecv.at[index, pair], z_sem.at[0, index, pair], z_sem.at[1, index, pair],
            device_id={"gz": around["gz"][sign]}, device_id_type=MESH,
        )

    def send_z(pair):
        for index in range(2):
            packed = None
            for half in range(2):
                for block in range(blocks):
                    place = 18 * (half * blocks + block)
                    value = zraw[index, 2 * pair + half, block]
                    packed = value if packed is None else jnp.where(lane >= place, pltpu.roll(value, place, 1), packed)
            zsend[index, pair] = packed
        for index in range(2):
            z_copy(pair, index).start()

    def merge_z(pair):
        for index, sign in enumerate((1, -1)):
            z_copy(pair, index).wait_recv()
            columns = zrecv[index, pair]
            for half in range(2):
                for block in range(blocks):
                    for member, offset in ZS[sign].items():
                        reach = abs(SPEEDS[member][2])
                        place = 18 * (half * blocks + block) + offset
                        target = 0 if sign > 0 else nz - reach
                        shift = (target - place) % nz
                        value = pltpu.roll(columns, shift, 1) if shift else columns
                        mask = lane < reach if sign > 0 else lane >= nz - reach
                        rows = row_of(member, 0, block)
                        pltpu.store(p_ref.at[member, 2 * pair + half, rows, :], value, mask=mask)

    halo = {1: up_ref, -1: down_ref}

    def x_copies(sign, members):
        copies = []
        for member in members:
            reach = abs(SPEEDS[member][0])
            rows = pl.ds(final_row(member), ny)
            layers = pl.ds(nx - reach, reach) if sign > 0 else pl.ds(0, reach)
            offset = XS[sign][member]
            place = list(XS[sign]).index(member)
            index = 0 if sign > 0 else 1
            copies.append(pltpu.make_async_remote_copy(
                p_ref.at[member, layers, rows, :], halo[sign].at[pl.ds(offset, reach), rows, :],
                x_sem.at[0, index, place], x_sem.at[1, index, place],
                device_id={"gx": around["gx"][sign]}, device_id_type=MESH,
            ))
        return copies

    def send_x(sign, members):
        for copy in x_copies(sign, members):
            copy.start()

    def d_copy(number):
        sx, sy = CORNERS[number]
        return pltpu.make_async_remote_copy(
            dsend.at[number], drecv.at[number], d_sem.at[0, number], d_sem.at[1, number],
            device_id={"gx": around["gx"][sx], "gy": around["gy"][sy]}, device_id_type=MESH,
        )

    def send_corners(sx):
        for number in range(4):
            if CORNERS[number][0] != sx:
                continue
            for place, (member, layer, row) in enumerate(corner_rows(*CORNERS[number])):
                x = nx - abs(SPEEDS[member][0]) + layer if sx > 0 else layer
                dsend[number, pl.ds(place, 1), :] = p_ref[member, x, pl.ds(leaving_row(member, row, ny), 1), :]
            d_copy(number).start()

    def y_copy(index):
        return pltpu.make_async_remote_copy(
            ysend.at[index], yrecv.at[index], y_sem.at[0, index], y_sem.at[1, index],
            device_id={"gy": around["gy"][(1, -1)[index]]}, device_id_type=MESH,
        )

    def send_y():
        for index, sign in enumerate((1, -1)):
            for member, offset in YS[sign].items():
                for row in range(abs(SPEEDS[member][1])):
                    ysend[index, offset + row] = read_rows(p_ref, member, leaving_row(member, row, ny))
            y_copy(index).start()

    def merge_y():
        for index, sign in enumerate((1, -1)):
            y_copy(index).wait_recv()
            for member, offset in YS[sign].items():
                for row in range(abs(SPEEDS[member][1])):
                    write_rows(p_ref, member, entering_row(member, row, ny), yrecv[index, offset + row])

    rate_load.wait()
    for turn, pair in enumerate(order):
        for copy in loads[pair]:
            copy.wait()
        collide_pair(pair)
        if turn == 0:
            pl.semaphore_wait(barrier, len(friends))
        send_z(pair)
        if turn == 0:
            send_x(1, EARLY[1])
        elif turn == 1:
            send_x(-1, EARLY[-1])
        elif pair == pairs - 2:
            send_x(1, THIRD[1])
        if pair == 1:
            send_x(-1, THIRD[-1])
    for turn, pair in enumerate(order):
        merge_z(pair)
        if turn < 2:
            sign = 1 if turn == 0 else -1
            send_x(sign, LATE[sign])
            send_corners(sign)
    send_y()
    for sign in (1, -1):
        for copy in x_copies(sign, list(XS[sign])):
            copy.wait_send()
    merge_y()
    for sign in (1, -1):
        for copy in x_copies(sign, list(XS[sign])):
            copy.wait_recv()
    for number, (sx, sy) in enumerate(CORNERS):
        d_copy(number).wait_recv()
        for place, (member, layer, row) in enumerate(corner_rows(sx, sy)):
            target = halo[sx]
            target[XS[sx][member] + layer, pl.ds(entering_row(member, row, ny), 1), :] = drecv[number, pl.ds(place, 1), :]
    for pair in order:
        for index in range(2):
            z_copy(pair, index).wait_send()
    for index in range(2):
        y_copy(index).wait_send()
    for number in range(4):
        d_copy(number).wait_send()


def emit_kernel(sizes, p_ref, up_ref, down_ref, o_hbm, sem):
    nx, ny, nz = sizes
    copies = []
    for member in range(Q):
        cx = SPEEDS[member][0]
        rows = pl.ds(final_row(member), ny)
        if cx > 0:
            pieces = [
                (p_ref.at[member, pl.ds(0, nx - cx), rows, :], o_hbm.at[member, pl.ds(cx, nx - cx)]),
                (up_ref.at[pl.ds(XS[1][member], cx), rows, :], o_hbm.at[member, pl.ds(0, cx)]),
            ]
        elif cx < 0:
            pieces = [
                (p_ref.at[member, pl.ds(-cx, nx + cx), rows, :], o_hbm.at[member, pl.ds(0, nx + cx)]),
                (down_ref.at[pl.ds(XS[-1][member], -cx), rows, :], o_hbm.at[member, pl.ds(nx + cx, -cx)]),
            ]
        else:
            pieces = [(p_ref.at[member, :, rows, :], o_hbm.at[member])]
        for source, target in pieces:
            copies.append(pltpu.make_async_copy(source, target, sem.at[len(copies)]))
    for copy in copies:
        copy.start()
    for copy in copies:
        copy.wait()


def per_device(populations, relax):
    sizes = populations.shape[1:]
    nx, ny, nz = sizes
    pairs, blocks = nx // 2, ny // 8
    vmem = pl.BlockSpec(memory_space=pltpu.VMEM)
    hbm = pl.BlockSpec(memory_space=pltpu.HBM)
    dma = pltpu.SemaphoreType.DMA
    shifted, up, down = pl.pallas_call(
        functools.partial(exchange_kernel, sizes),
        out_shape=(
            jax.ShapeDtypeStruct((Q, nx, ROWS, nz), F32),
            jax.ShapeDtypeStruct((18, ROWS, nz), F32),
            jax.ShapeDtypeStruct((18, ROWS, nz), F32),
        ),
        in_specs=[hbm, hbm],
        out_specs=(vmem, vmem, vmem),
        scratch_shapes=[
            pltpu.VMEM((Q, nx, ny, nz), F32),
            pltpu.VMEM((nx, ny, nz), F32),
            pltpu.VMEM((2, nx, blocks, 8, nz), F32),
            pltpu.VMEM((2, pairs, 8, nz), F32),
            pltpu.VMEM((2, pairs, 8, nz), F32),
            pltpu.VMEM((2, 18, nx, nz), F32),
            pltpu.VMEM((2, 18, nx, nz), F32),
            pltpu.VMEM((4, 8, nz), F32),
            pltpu.VMEM((4, 8, nz), F32),
            dma((pairs + 1,)),
            dma((2, 2, pairs)),
            dma((2, 2)),
            dma((2, 4)),
            dma((2, 2, 11)),
        ],
        compiler_params=pltpu.CompilerParams(
            collective_id=0, has_side_effects=True, vmem_limit_bytes=24 * 1024 * 1024
        ),
        name="collide_exchange",
    )(*(pltpu.with_memory_space_constraint(array, pltpu.HBM) for array in (populations, relax)))
    return pl.pallas_call(
        functools.partial(emit_kernel, sizes),
        out_shape=jax.ShapeDtypeStruct(populations.shape, F32),
        in_specs=[vmem, vmem, vmem],
        out_specs=hbm,
        scratch_shapes=[dma((61,))],
        compiler_params=pltpu.CompilerParams(vmem_limit_bytes=24 * 1024 * 1024),
        name="emit",
    )(shifted, up, down)


def solution(mesh):
    return jax.shard_map(
        per_device,
        mesh=mesh,
        in_specs=(P(None, "gx", "gy", "gz"), P("gx", "gy", "gz")),
        out_specs=P(None, "gx", "gy", "gz"),
        check_vma=False,
    )
```

```python
import functools

import jax
import jax.numpy as jnp
from jax import lax
from jax.experimental import pallas as pl
from jax.experimental.pallas import tpu as pltpu
from jax.sharding import PartitionSpec as P

MESH = pl.DeviceIdType.MESH
F32 = jnp.float32


def lattice():
    speeds = [(0, 0, 0)]
    weights = [1.0 / 12.0]
    for axis in range(3):
        for sign in (1, -1):
            vector = [0, 0, 0]
            vector[axis] = sign
            speeds.append(tuple(vector))
            weights.append(1.0 / 12.0)
    for first in (1, -1):
        for second in (1, -1):
            for third in (1, -1):
                speeds.append((first, second, third))
                weights.append(1.0 / 27.0)
    for axis in range(3):
        for sign in (2, -2):
            vector = [0, 0, 0]
            vector[axis] = sign
            speeds.append(tuple(vector))
            weights.append(2.0 / 135.0)
    for couple in ((0, 1), (0, 2), (1, 2)):
        for first in (2, -2):
            for second in (2, -2):
                vector = [0, 0, 0]
                vector[couple[0]] = first
                vector[couple[1]] = second
                speeds.append(tuple(vector))
                weights.append(1.0 / 432.0)
    for axis in range(3):
        for sign in (3, -3):
            vector = [0, 0, 0]
            vector[axis] = sign
            speeds.append(tuple(vector))
            weights.append(1.0 / 1620.0)
    return speeds, weights


SPEEDS, WEIGHTS = lattice()
Q = 39
INDEX = {vector: member for member, vector in enumerate(SPEEDS)}
ROWS = 32


def slots(axis, sign):
    table, offset = {}, 0
    for third in (0, 1, -1):
        for member in range(Q):
            speed = SPEEDS[member][axis] * sign
            cz = SPEEDS[member][2] if axis < 2 else 0
            if speed > 0 and (cz > 0) - (cz < 0) == third:
                table[member] = offset
                offset += speed
    return table


XS = {sign: slots(0, sign) for sign in (1, -1)}
YS = {sign: slots(1, sign) for sign in (1, -1)}
ZS = {sign: slots(2, sign) for sign in (1, -1)}
FLAT = {sign: [m for m in XS[sign] if SPEEDS[m][2] == 0] for sign in (1, -1)}
TILTED = {sign: [m for m in XS[sign] if SPEEDS[m][2] != 0] for sign in (1, -1)}
EDGE = 4
CORNERS = [(1, 1), (1, -1), (-1, 1), (-1, -1)]
SHELLS = {0.0: "0", 1.0: "1", 3.0: "c", 4.0: "2", 8.0: "e", 9.0: "3"}


def square(member):
    return float(sum(value * value for value in SPEEDS[member]))


def final_row(member):
    return 8 if SPEEDS[member][1] < 0 else 0


def corner_rows(sx, sy):
    rows = []
    for member in range(Q):
        cx, cy = SPEEDS[member][0] * sx, SPEEDS[member][1] * sy
        if cx > 0 and cy > 0:
            rows += [(member, layer, row) for layer in range(cx) for row in range(cy)]
    return rows


def leaving_row(member, row, ny):
    cy = SPEEDS[member][1]
    return ny + row if cy > 0 else 8 + cy + row


def entering_row(member, row, ny):
    cy = SPEEDS[member][1]
    return row if cy > 0 else 8 + ny + cy + row


def strided(ref, member, row):
    count, layers, rows, lanes = ref.shape
    return ref.reshape(count * layers * rows, lanes), pl.ds(member * layers * rows + row, layers, stride=rows)


def read_rows(ref, member, row):
    flat, where = strided(ref, member, row)
    return flat[where, :]


def write_rows(ref, member, row, value):
    flat, where = strided(ref, member, row)
    flat[where, :] = value


def collide(load, rate, store):
    weight = {shell: WEIGHTS[m] for m in range(Q) for shell in [SHELLS[square(m)]]}
    total = {}
    odd = {}
    for member in range(Q):
        vector = SPEEDS[member]
        shell = SHELLS[square(member)]
        opposite = INDEX[tuple(-value for value in vector)]
        if member == opposite:
            total[shell] = load(member)
        elif member < opposite:
            one, other = load(member), load(opposite)
            both = one + other
            total[shell] = total[shell] + both if shell in total else both
            odd[member] = one - other
    density = sum(weight[shell] * total[shell] for shell in total)
    energy = sum(weight[SHELLS[v]] * v * total[SHELLS[v]] for v in (1.0, 3.0, 4.0, 8.0, 9.0))
    inverse = 1.0 / density
    drift = []
    for axis in range(3):
        parts = {}
        for member, value in odd.items():
            speed = SPEEDS[member][axis]
            if speed == 0:
                continue
            key = (SHELLS[square(member)], abs(speed))
            if key in parts:
                parts[key] = parts[key] + value if speed > 0 else parts[key] - value
            else:
                parts[key] = value if speed > 0 else -value
        flux = sum((weight[shell] * speed * 1.5) * value for (shell, speed), value in parts.items())
        drift.append(flux * inverse)
    w = drift
    ww = [value * value for value in w]
    norm = (ww[0] + ww[1] + ww[2]) * (4.0 / 9.0)
    t = (energy * inverse - norm) * 0.5 - 1.0
    b = 1.5 * norm
    scale = rate * density
    keep = 1.0 - rate
    tb = t * b
    t2 = t * t
    p0 = scale * (1.0 - 0.5 * b + 0.125 * b * b - 1.5 * t + 1.25 * tb + 1.875 * t2)
    p1 = scale * (0.5 * t - 0.25 * tb - 1.25 * t2)
    p2 = scale * (0.125 * t2)
    st = scale * t
    b0 = scale * (0.5 - 0.25 * b) - 1.75 * st
    c0 = scale * (1.0 - 0.5 * b) - 2.5 * st
    quart = {k: (k**4 / 24.0) * scale for k in (1, 2, 3)}
    cubic = {k: (k**3 / 6.0) * scale for k in (1, 2, 3)}
    reach = {"1": 1, "c": 1, "2": 2, "e": 2, "3": 3}
    coefficients = {}
    for value, shell in SHELLS.items():
        s = 1.5 * value
        even = p0 + s * p1 + (s * s) * p2 if s else p0
        if s:
            k = reach[shell]
            coefficients[shell] = (
                even,
                (k * k) * b0 + (k * k * s * 0.25) * st,
                k * c0 + (k * s * 0.5) * st,
                quart[k],
                cubic[k],
            )
        else:
            coefficients[shell] = even
    for member in range(Q):
        vector = SPEEDS[member]
        shell = SHELLS[square(member)]
        opposite = INDEX[tuple(-value for value in vector)]
        if member == opposite:
            store(member, keep * load(member) + coefficients[shell])
        elif member < opposite:
            k = reach[shell]
            q, q2 = None, None
            axes = [axis for axis in range(3) if vector[axis] != 0]
            if len(axes) == 1:
                q, q2 = w[axes[0]], ww[axes[0]]
            else:
                q = w[axes[0]]
                for axis in axes[1:]:
                    q = q + w[axis] if vector[axis] > 0 else q - w[axis]
                q2 = q * q
            e0, e2, o1, e4, o3 = coefficients[shell]
            even = e0 + q2 * (e2 + q2 * e4)
            uneven = q * (o1 + q2 * o3)
            store(member, keep * load(member) + (even + uneven))
            store(opposite, keep * load(opposite) + (even - uneven))


def exchange_kernel(
    sizes, g_hbm, r_hbm, p_ref, up_ref, down_ref,
    g, rate, zraw, zsend, zrecv, xzrecv, ysend, yrecv, yzrecv, dsend, drecv, dzrecv,
    load_sem, z_sem, xz_sem, y_sem, yz_sem, d_sem, dz_sem, x_sem, ready_sem, far_sem,
):
    nx, ny, nz = sizes
    blocks = ny // 8
    signs = (1, -1)
    around = {}
    for axis in ("gx", "gy", "gz"):
        me, count = lax.axis_index(axis), lax.axis_size(axis)
        around[axis] = {1: lax.rem(me + 1, count), -1: lax.rem(me + count - 1, count)}

    def layer_load(x):
        return pltpu.make_async_copy(g_hbm.at[:, pl.ds(x, 1)], g.at[:, pl.ds(x, 1)], load_sem.at[x])

    rate_load = pltpu.make_async_copy(r_hbm, rate, load_sem.at[nx])
    rate_load.start()
    for x in range(nx):
        layer_load(x).start()

    barrier = pltpu.get_barrier_semaphore()
    for axis in ("gx", "gy", "gz"):
        for sign in signs:
            pl.semaphore_signal(barrier, inc=1, device_id={axis: around[axis][sign]}, device_id_type=MESH)

    lane = lax.broadcasted_iota(jnp.int32, (8, nz), 1)
    pack_masks = {offset: lane >= offset for offset in sorted(set(ZS[1].values())) if offset}

    def row_of(member, block):
        return pl.ds(final_row(member) + SPEEDS[member][1] + 8 * block, 8)

    def collide_block(x, block):
        pieces = {1: {}, -1: {}}

        def load(member):
            return g[member, x, pl.ds(8 * block, 8), :]

        def store(member, value):
            cz = SPEEDS[member][2]
            if cz != 0:
                p_ref[member, x, row_of(member, block), :] = pltpu.roll(value, cz % nz, 1)
                sign = 1 if cz > 0 else -1
                place = ZS[sign][member]
                shift = (place + max(cz, 0)) % nz
                pieces[sign][place] = pltpu.roll(value, shift, 1) if shift else value
            else:
                p_ref[member, x, row_of(member, block), :] = value

        collide(load, rate[x, pl.ds(8 * block, 8), :], store)
        for index, sign in enumerate(signs):
            packed = None
            for place in sorted(pieces[sign]):
                packed = pieces[sign][place] if packed is None else jnp.where(pack_masks[place], pieces[sign][place], packed)
            zraw[index, x, block] = packed

    def collide_layer(x, carry):
        layer_load(x).wait()
        for block in range(blocks):
            collide_block(x, block)
        return carry

    def column(half, block, offset):
        return 18 * (half * blocks + block) + offset

    def fold_z(index, pair):
        packed = None
        for half in range(2):
            for block in range(blocks):
                place = column(half, block, 0)
                value = zraw[index, 2 * pair + half, block]
                packed = value if packed is None else jnp.where(lane >= place, pltpu.roll(value, place, 1), packed)
        zsend[index, pair] = packed

    def enters(sign, reach):
        return lane < reach if sign > 0 else lane >= nz - reach

    def unfold(columns, target, member, half, block, rows):
        cz = SPEEDS[member][2]
        sign, reach = (1, cz) if cz > 0 else (-1, -cz)
        place = column(half, block, ZS[sign][member])
        shift = ((0 if sign > 0 else nz - reach) - place) % nz
        value = pltpu.roll(columns, shift, 1) if shift else columns
        pltpu.store(target.at[rows, :], value, mask=enters(sign, reach))

    def z_copy(index):
        return pltpu.make_async_remote_copy(
            zsend.at[index], zrecv.at[index], z_sem.at[0, index], z_sem.at[1, index],
            device_id={"gz": around["gz"][signs[index]]}, device_id_type=MESH,
        )

    def xz_copy(ix, iz):
        pair = nx // 2 - 1 if ix == 0 else 0
        return pltpu.make_async_remote_copy(
            zsend.at[iz, pair], xzrecv.at[ix, iz], xz_sem.at[0, ix, iz], xz_sem.at[1, ix, iz],
            device_id={"gx": around["gx"][signs[ix]], "gz": around["gz"][signs[iz]]}, device_id_type=MESH,
        )

    halo = (up_ref, down_ref)

    def x_copy(ix, member):
        sign, reach = signs[ix], abs(SPEEDS[member][0])
        rows = pl.ds(final_row(member), ny)
        layers = pl.ds(nx - reach, reach) if sign > 0 else pl.ds(0, reach)
        place = list(XS[sign]).index(member)
        return pltpu.make_async_remote_copy(
            p_ref.at[member, layers, rows, :], halo[ix].at[pl.ds(XS[sign][member], reach), rows, :],
            x_sem.at[0, ix, place], x_sem.at[1, ix, place],
            device_id={"gx": around["gx"][sign]}, device_id_type=MESH,
        )

    def d_copy(number):
        sx, sy = CORNERS[number]
        return pltpu.make_async_remote_copy(
            dsend.at[number], drecv.at[number], d_sem.at[0, number], d_sem.at[1, number],
            device_id={"gx": around["gx"][sx], "gy": around["gy"][sy]}, device_id_type=MESH,
        )

    def dz_copy(number, iz):
        sx, sy = CORNERS[number]
        return pltpu.make_async_remote_copy(
            dsend.at[number], dzrecv.at[number, iz], dz_sem.at[0, number, iz], dz_sem.at[1, number, iz],
            device_id={"gx": around["gx"][sx], "gy": around["gy"][sy], "gz": around["gz"][signs[iz]]},
            device_id_type=MESH,
        )

    def y_copy(iy):
        return pltpu.make_async_remote_copy(
            ysend.at[iy], yrecv.at[iy], y_sem.at[0, iy], y_sem.at[1, iy],
            device_id={"gy": around["gy"][signs[iy]]}, device_id_type=MESH,
        )

    def yz_copy(iy, iz):
        return pltpu.make_async_remote_copy(
            ysend.at[iy, pl.ds(18 - (2 - iz) * EDGE, EDGE)], yzrecv.at[iy, iz],
            yz_sem.at[0, iy, iz], yz_sem.at[1, iy, iz],
            device_id={"gy": around["gy"][signs[iy]], "gz": around["gz"][signs[iz]]}, device_id_type=MESH,
        )

    rate_load.wait()
    lax.fori_loop(0, nx, collide_layer, 0)
    pl.semaphore_wait(barrier, 6)
    for axis in ("gy", "gz"):
        for sign in signs:
            pl.semaphore_signal(ready_sem, inc=1, device_id={axis: around[axis][sign]}, device_id_type=MESH)
    for members in (TILTED, FLAT):
        for ix, sign in enumerate(signs):
            for member in members[sign]:
                x_copy(ix, member).start()
    for index in range(2):
        for pair in range(nx // 2):
            fold_z(index, pair)
    for index in range(2):
        z_copy(index).start()
    for iy, sign in enumerate(signs):
        for member, offset in YS[sign].items():
            for row in range(abs(SPEEDS[member][1])):
                ysend[iy, offset + row] = read_rows(p_ref, member, leaving_row(member, row, ny))
        y_copy(iy).start()
    for number, (sx, sy) in enumerate(CORNERS):
        for place, (member, layer, row) in enumerate(corner_rows(sx, sy)):
            x = nx - abs(SPEEDS[member][0]) + layer if sx > 0 else layer
            dsend[number, pl.ds(place, 1), :] = p_ref[member, x, pl.ds(leaving_row(member, row, ny), 1), :]
    pl.semaphore_wait(ready_sem, 4)
    for sign in signs:
        pl.semaphore_signal(far_sem, inc=1, device_id={"gz": around["gz"][sign]}, device_id_type=MESH)
    for number in range(4):
        d_copy(number).start()
    for ix in range(2):
        for iz in range(2):
            xz_copy(ix, iz).start()
    for iy in range(2):
        for iz in range(2):
            yz_copy(iy, iz).start()
    pl.semaphore_wait(far_sem, 2)
    for number in range(4):
        for iz in range(2):
            dz_copy(number, iz).start()

    def merge_z(index, wanted):
        for pair in range(nx // 2):
            columns = zrecv[index, pair]
            for half in range(2):
                for block in range(blocks):
                    for member in ZS[signs[index]]:
                        x = 2 * pair + half
                        if wanted(member, x):
                            unfold(columns, p_ref.at[member, x], member, half, block, row_of(member, block))

    def travels(member, x):
        cx = SPEEDS[member][0]
        return x >= nx - cx if cx > 0 else x < -cx

    for index in range(2):
        z_copy(index).wait_recv()
        merge_z(index, lambda member, x: not travels(member, x))
    for members in (TILTED, FLAT):
        for ix, sign in enumerate(signs):
            for member in members[sign]:
                x_copy(ix, member).wait_send()
    for index in range(2):
        merge_z(index, travels)
    for iy, sign in enumerate(signs):
        y_copy(iy).wait_recv()
        for iz in range(2):
            yz_copy(iy, iz).wait_recv()
        for member, offset in YS[sign].items():
            cz = SPEEDS[member][2]
            for row in range(abs(SPEEDS[member][1])):
                value = yrecv[iy, offset + row]
                if cz != 0:
                    iz = 0 if cz > 0 else 1
                    edge = yzrecv[iy, iz, offset + row - 18 + (2 - iz) * EDGE]
                    value = jnp.where(enters(signs[iz], abs(cz)), edge, value)
                write_rows(p_ref, member, entering_row(member, row, ny), value)
    for ix, sign in enumerate(signs):
        for iz in range(2):
            xz_copy(ix, iz).wait_recv()
        for member in TILTED[sign]:
            x_copy(ix, member).wait_recv()
            reach, iz = abs(SPEEDS[member][0]), 0 if SPEEDS[member][2] > 0 else 1
            for layer in range(reach):
                half = 2 - reach + layer if sign > 0 else layer
                for block in range(blocks):
                    target = halo[ix].at[XS[sign][member] + layer]
                    unfold(xzrecv[ix, iz], target, member, half, block, row_of(member, block))
    for ix, sign in enumerate(signs):
        for member in FLAT[sign]:
            x_copy(ix, member).wait_recv()
    for number, (sx, sy) in enumerate(CORNERS):
        ix = 0 if sx > 0 else 1
        d_copy(number).wait_recv()
        for iz in range(2):
            dz_copy(number, iz).wait_recv()
        for place, (member, layer, row) in enumerate(corner_rows(sx, sy)):
            cz = SPEEDS[member][2]
            value = drecv[number, pl.ds(place, 1), :]
            if cz != 0:
                iz = 0 if cz > 0 else 1
                mask = enters(signs[iz], abs(cz))[:1]
                value = jnp.where(mask, dzrecv[number, iz, pl.ds(place, 1), :], value)
            halo[ix][XS[sx][member] + layer, pl.ds(entering_row(member, row, ny), 1), :] = value
    for index in range(2):
        z_copy(index).wait_send()
        y_copy(index).wait_send()
        for iz in range(2):
            xz_copy(index, iz).wait_send()
            yz_copy(index, iz).wait_send()
    for number in range(4):
        d_copy(number).wait_send()
        for iz in range(2):
            dz_copy(number, iz).wait_send()


def emit_kernel(sizes, p_ref, up_ref, down_ref, o_hbm, sem):
    nx, ny, nz = sizes
    copies = []
    for member in range(Q):
        cx = SPEEDS[member][0]
        rows = pl.ds(final_row(member), ny)
        if cx > 0:
            pieces = [
                (p_ref.at[member, pl.ds(0, nx - cx), rows, :], o_hbm.at[member, pl.ds(cx, nx - cx)]),
                (up_ref.at[pl.ds(XS[1][member], cx), rows, :], o_hbm.at[member, pl.ds(0, cx)]),
            ]
        elif cx < 0:
            pieces = [
                (p_ref.at[member, pl.ds(-cx, nx + cx), rows, :], o_hbm.at[member, pl.ds(0, nx + cx)]),
                (down_ref.at[pl.ds(XS[-1][member], -cx), rows, :], o_hbm.at[member, pl.ds(nx + cx, -cx)]),
            ]
        else:
            pieces = [(p_ref.at[member, :, rows, :], o_hbm.at[member])]
        for source, target in pieces:
            copies.append(pltpu.make_async_copy(source, target, sem.at[len(copies)]))
    for copy in copies:
        copy.start()
    for copy in copies:
        copy.wait()


def per_device(populations, relax):
    sizes = populations.shape[1:]
    nx, ny, nz = sizes
    blocks = ny // 8
    vmem = pl.BlockSpec(memory_space=pltpu.VMEM)
    hbm = pl.BlockSpec(memory_space=pltpu.HBM)
    dma = pltpu.SemaphoreType.DMA
    shifted, up, down = pl.pallas_call(
        functools.partial(exchange_kernel, sizes),
        out_shape=(
            jax.ShapeDtypeStruct((Q, nx, ROWS, nz), F32),
            jax.ShapeDtypeStruct((18, ROWS, nz), F32),
            jax.ShapeDtypeStruct((18, ROWS, nz), F32),
        ),
        in_specs=[hbm, hbm],
        out_specs=(vmem, vmem, vmem),
        scratch_shapes=[
            pltpu.VMEM((Q, nx, ny, nz), F32),
            pltpu.VMEM((nx, ny, nz), F32),
            pltpu.VMEM((2, nx, blocks, 8, nz), F32),
            pltpu.VMEM((2, nx // 2, 8, nz), F32),
            pltpu.VMEM((2, nx // 2, 8, nz), F32),
            pltpu.VMEM((2, 2, 8, nz), F32),
            pltpu.VMEM((2, 18, nx, nz), F32),
            pltpu.VMEM((2, 18, nx, nz), F32),
            pltpu.VMEM((2, 2, EDGE, nx, nz), F32),
            pltpu.VMEM((4, 8, nz), F32),
            pltpu.VMEM((4, 8, nz), F32),
            pltpu.VMEM((4, 2, 8, nz), F32),
            dma((nx + 1,)),
            dma((2, 2)),
            dma((2, 2, 2)),
            dma((2, 2)),
            dma((2, 2, 2)),
            dma((2, 4)),
            dma((2, 4, 2)),
            dma((2, 2, 11)),
            pltpu.SemaphoreType.REGULAR,
            pltpu.SemaphoreType.REGULAR,
        ],
        compiler_params=pltpu.CompilerParams(
            collective_id=0, has_side_effects=True, vmem_limit_bytes=24 * 1024 * 1024
        ),
        name="collide_exchange",
    )(*(pltpu.with_memory_space_constraint(array, pltpu.HBM) for array in (populations, relax)))
    return pl.pallas_call(
        functools.partial(emit_kernel, sizes),
        out_shape=jax.ShapeDtypeStruct(populations.shape, F32),
        in_specs=[vmem, vmem, vmem],
        out_specs=hbm,
        scratch_shapes=[dma((61,))],
        compiler_params=pltpu.CompilerParams(vmem_limit_bytes=24 * 1024 * 1024),
        name="emit",
    )(shifted, up, down)


def solution(mesh):
    return jax.shard_map(
        per_device,
        mesh=mesh,
        in_specs=(P(None, "gx", "gy", "gz"), P("gx", "gy", "gz")),
        out_specs=P(None, "gx", "gy", "gz"),
        check_vma=False,
    )
```

```python
import functools

import jax
import jax.numpy as jnp
from jax import lax
from jax.experimental import pallas as pl
from jax.experimental.pallas import tpu as pltpu
from jax.sharding import PartitionSpec as P

MESH = pl.DeviceIdType.MESH
F32 = jnp.float32


def lattice():
    speeds = [(0, 0, 0)]
    weights = [1.0 / 12.0]
    for axis in range(3):
        for sign in (1, -1):
            vector = [0, 0, 0]
            vector[axis] = sign
            speeds.append(tuple(vector))
            weights.append(1.0 / 12.0)
    for first in (1, -1):
        for second in (1, -1):
            for third in (1, -1):
                speeds.append((first, second, third))
                weights.append(1.0 / 27.0)
    for axis in range(3):
        for sign in (2, -2):
            vector = [0, 0, 0]
            vector[axis] = sign
            speeds.append(tuple(vector))
            weights.append(2.0 / 135.0)
    for couple in ((0, 1), (0, 2), (1, 2)):
        for first in (2, -2):
            for second in (2, -2):
                vector = [0, 0, 0]
                vector[couple[0]] = first
                vector[couple[1]] = second
                speeds.append(tuple(vector))
                weights.append(1.0 / 432.0)
    for axis in range(3):
        for sign in (3, -3):
            vector = [0, 0, 0]
            vector[axis] = sign
            speeds.append(tuple(vector))
            weights.append(1.0 / 1620.0)
    return speeds, weights


SPEEDS, WEIGHTS = lattice()
Q = 39
INDEX = {vector: member for member, vector in enumerate(SPEEDS)}
ROWS = 32


def slots(axis, sign):
    table, offset = {}, 0
    for third in (0, 1, -1):
        for member in range(Q):
            speed = SPEEDS[member][axis] * sign
            cz = SPEEDS[member][2] if axis < 2 else 0
            if speed > 0 and (cz > 0) - (cz < 0) == third:
                table[member] = offset
                offset += speed
    return table


XS = {sign: slots(0, sign) for sign in (1, -1)}
YS = {sign: slots(1, sign) for sign in (1, -1)}
ZS = {sign: slots(2, sign) for sign in (1, -1)}
FLAT = {sign: [m for m in XS[sign] if SPEEDS[m][2] == 0] for sign in (1, -1)}
TILTED = {sign: [m for m in XS[sign] if SPEEDS[m][2] != 0] for sign in (1, -1)}
EDGE = 4
CORNERS = [(1, 1), (1, -1), (-1, 1), (-1, -1)]
SHELLS = {0.0: "0", 1.0: "1", 3.0: "c", 4.0: "2", 8.0: "e", 9.0: "3"}


def square(member):
    return float(sum(value * value for value in SPEEDS[member]))


def final_row(member):
    return 8 if SPEEDS[member][1] < 0 else 0


def corner_rows(sx, sy):
    rows = []
    for member in range(Q):
        cx, cy = SPEEDS[member][0] * sx, SPEEDS[member][1] * sy
        if cx > 0 and cy > 0:
            rows += [(member, layer, row) for layer in range(cx) for row in range(cy)]
    return rows


def leaving_row(member, row, ny):
    cy = SPEEDS[member][1]
    return ny + row if cy > 0 else 8 + cy + row


def entering_row(member, row, ny):
    cy = SPEEDS[member][1]
    return row if cy > 0 else 8 + ny + cy + row


def strided(ref, member, row):
    count, layers, rows, lanes = ref.shape
    return ref.reshape(count * layers * rows, lanes), pl.ds(member * layers * rows + row, layers, stride=rows)


def read_rows(ref, member, row):
    flat, where = strided(ref, member, row)
    return flat[where, :]


def write_rows(ref, member, row, value):
    flat, where = strided(ref, member, row)
    flat[where, :] = value


def collide(load, rate, store):
    weight = {shell: WEIGHTS[m] for m in range(Q) for shell in [SHELLS[square(m)]]}
    total = {}
    odd = {}
    for member in range(Q):
        vector = SPEEDS[member]
        shell = SHELLS[square(member)]
        opposite = INDEX[tuple(-value for value in vector)]
        if member == opposite:
            total[shell] = load(member)
        elif member < opposite:
            one, other = load(member), load(opposite)
            both = one + other
            total[shell] = total[shell] + both if shell in total else both
            odd[member] = one - other
    density = sum(weight[shell] * total[shell] for shell in total)
    energy = sum(weight[SHELLS[v]] * v * total[SHELLS[v]] for v in (1.0, 3.0, 4.0, 8.0, 9.0))
    inverse = 1.0 / density
    drift = []
    for axis in range(3):
        parts = {}
        for member, value in odd.items():
            speed = SPEEDS[member][axis]
            if speed == 0:
                continue
            key = (SHELLS[square(member)], abs(speed))
            if key in parts:
                parts[key] = parts[key] + value if speed > 0 else parts[key] - value
            else:
                parts[key] = value if speed > 0 else -value
        flux = sum((weight[shell] * speed * 1.5) * value for (shell, speed), value in parts.items())
        drift.append(flux * inverse)
    w = drift
    ww = [value * value for value in w]
    norm = (ww[0] + ww[1] + ww[2]) * (4.0 / 9.0)
    t = (energy * inverse - norm) * 0.5 - 1.0
    b = 1.5 * norm
    scale = rate * density
    keep = 1.0 - rate
    tb = t * b
    t2 = t * t
    p0 = scale * (1.0 - 0.5 * b + 0.125 * b * b - 1.5 * t + 1.25 * tb + 1.875 * t2)
    p1 = scale * (0.5 * t - 0.25 * tb - 1.25 * t2)
    p2 = scale * (0.125 * t2)
    st = scale * t
    b0 = scale * (0.5 - 0.25 * b) - 1.75 * st
    c0 = scale * (1.0 - 0.5 * b) - 2.5 * st
    quart = {k: (k**4 / 24.0) * scale for k in (1, 2, 3)}
    cubic = {k: (k**3 / 6.0) * scale for k in (1, 2, 3)}
    reach = {"1": 1, "c": 1, "2": 2, "e": 2, "3": 3}
    coefficients = {}
    for value, shell in SHELLS.items():
        s = 1.5 * value
        even = p0 + s * p1 + (s * s) * p2 if s else p0
        if s:
            k = reach[shell]
            coefficients[shell] = (
                even,
                (k * k) * b0 + (k * k * s * 0.25) * st,
                k * c0 + (k * s * 0.5) * st,
                quart[k],
                cubic[k],
            )
        else:
            coefficients[shell] = even
    for member in range(Q):
        vector = SPEEDS[member]
        shell = SHELLS[square(member)]
        opposite = INDEX[tuple(-value for value in vector)]
        if member == opposite:
            store(member, keep * load(member) + coefficients[shell])
        elif member < opposite:
            k = reach[shell]
            q, q2 = None, None
            axes = [axis for axis in range(3) if vector[axis] != 0]
            if len(axes) == 1:
                q, q2 = w[axes[0]], ww[axes[0]]
            else:
                q = w[axes[0]]
                for axis in axes[1:]:
                    q = q + w[axis] if vector[axis] > 0 else q - w[axis]
                q2 = q * q
            e0, e2, o1, e4, o3 = coefficients[shell]
            even = e0 + q2 * (e2 + q2 * e4)
            uneven = q * (o1 + q2 * o3)
            store(member, keep * load(member) + (even + uneven))
            store(opposite, keep * load(opposite) + (even - uneven))


def exchange_kernel(
    sizes, g_hbm, r_hbm, p_ref, up_ref, down_ref,
    g, rate, zraw, zsend, zrecv, xzrecv, ysend, yrecv, yzrecv, dsend, drecv, dzrecv,
    load_sem, z_sem, xz_sem, y_sem, yz_sem, d_sem, dz_sem, x_sem, pair_sem, plane_sem, ready_sem,
):
    nx, ny, nz = sizes
    blocks = ny // 8
    signs = (1, -1)
    around = {}
    for axis in ("gx", "gy", "gz"):
        me, count = lax.axis_index(axis), lax.axis_size(axis)
        around[axis] = {1: lax.rem(me + 1, count), -1: lax.rem(me + count - 1, count)}

    def layer_load(x):
        return pltpu.make_async_copy(g_hbm.at[:, pl.ds(x, 1)], g.at[:, pl.ds(x, 1)], load_sem.at[x])

    rate_load = pltpu.make_async_copy(r_hbm, rate, load_sem.at[nx])
    rate_load.start()
    for x in [nx - 1, nx - 2, 0, 1] + list(range(2, nx - 2)):
        layer_load(x).start()

    barrier = pltpu.get_barrier_semaphore()
    gz = lax.axis_index("gz")
    core = lax.rem(gz, 2)
    chip = gz - core
    other_chip = lax.rem(chip + 2, lax.axis_size("gz"))
    partner = chip + 1 - core

    def tell(semaphore, **device):
        pl.semaphore_signal(semaphore, inc=1, device_id=device, device_id_type=MESH)

    for sign in signs:
        tell(barrier, gx=around["gx"][sign], gz=chip)
        tell(barrier, gy=around["gy"][sign], gz=chip + 1)
    tell(barrier, gz=other_chip)

    tell(barrier, gz=partner)

    lane = lax.broadcasted_iota(jnp.int32, (8, nz), 1)
    pack_masks = {offset: lane >= offset for offset in sorted(set(ZS[1].values())) if offset}

    def row_of(member, block):
        return pl.ds(final_row(member) + SPEEDS[member][1] + 8 * block, 8)

    def collide_block(x, block):
        pieces = {1: {}, -1: {}}

        def load(member):
            return g[member, x, pl.ds(8 * block, 8), :]

        def store(member, value):
            cz = SPEEDS[member][2]
            if cz != 0:
                p_ref[member, x, row_of(member, block), :] = pltpu.roll(value, cz % nz, 1)
                sign = 1 if cz > 0 else -1
                place = ZS[sign][member]
                shift = (place + max(cz, 0)) % nz
                pieces[sign][place] = pltpu.roll(value, shift, 1) if shift else value
            else:
                p_ref[member, x, row_of(member, block), :] = value

        collide(load, rate[x, pl.ds(8 * block, 8), :], store)
        for index, sign in enumerate(signs):
            packed = None
            for place in sorted(pieces[sign]):
                packed = pieces[sign][place] if packed is None else jnp.where(pack_masks[place], pieces[sign][place], packed)
            zraw[index, x, block] = packed

    def collide_layer(x, carry):
        layer_load(x).wait()
        for block in range(blocks):
            collide_block(x, block)
        return carry

    def column(half, block, offset):
        return 18 * (half * blocks + block) + offset

    def fold_z(index, pair):
        packed = None
        for half in range(2):
            for block in range(blocks):
                place = column(half, block, 0)
                value = zraw[index, 2 * pair + half, block]
                packed = value if packed is None else jnp.where(lane >= place, pltpu.roll(value, place, 1), packed)
        zsend[index, pair] = packed

    def enters(sign, reach):
        return lane < reach if sign > 0 else lane >= nz - reach

    def unfold(columns, target, member, half, block, rows):
        cz = SPEEDS[member][2]
        sign, reach = (1, cz) if cz > 0 else (-1, -cz)
        place = column(half, block, ZS[sign][member])
        shift = ((0 if sign > 0 else nz - reach) - place) % nz
        value = pltpu.roll(columns, shift, 1) if shift else columns
        pltpu.store(target.at[rows, :], value, mask=enters(sign, reach))

    def z_copy(index):
        return pltpu.make_async_remote_copy(
            zsend.at[index], zrecv.at[index], z_sem.at[0, index], z_sem.at[1, index],
            device_id={"gz": around["gz"][signs[index]]}, device_id_type=MESH,
        )

    def xz_copy(ix, iz):
        pair = nx // 2 - 1 if ix == 0 else 0
        return pltpu.make_async_remote_copy(
            zsend.at[iz, pair], xzrecv.at[ix, iz], xz_sem.at[0, ix, iz], xz_sem.at[1, ix, iz],
            device_id={"gx": around["gx"][signs[ix]], "gz": around["gz"][signs[iz]]}, device_id_type=MESH,
        )

    halo = (up_ref, down_ref)

    def x_copy(ix, member):
        sign, reach = signs[ix], abs(SPEEDS[member][0])
        rows = pl.ds(final_row(member), ny)
        layers = pl.ds(nx - reach, reach) if sign > 0 else pl.ds(0, reach)
        place = list(XS[sign]).index(member)
        return pltpu.make_async_remote_copy(
            p_ref.at[member, layers, rows, :], halo[ix].at[pl.ds(XS[sign][member], reach), rows, :],
            x_sem.at[0, ix, place], x_sem.at[1, ix, place],
            device_id={"gx": around["gx"][sign]}, device_id_type=MESH,
        )

    def d_copy(number):
        sx, sy = CORNERS[number]
        return pltpu.make_async_remote_copy(
            dsend.at[number], drecv.at[number], d_sem.at[0, number], d_sem.at[1, number],
            device_id={"gx": around["gx"][sx], "gy": around["gy"][sy]}, device_id_type=MESH,
        )

    def dz_copy(number, iz):
        sx, sy = CORNERS[number]
        return pltpu.make_async_remote_copy(
            dsend.at[number], dzrecv.at[number, iz], dz_sem.at[0, number, iz], dz_sem.at[1, number, iz],
            device_id={"gx": around["gx"][sx], "gy": around["gy"][sy], "gz": around["gz"][signs[iz]]},
            device_id_type=MESH,
        )

    def y_copy(iy):
        return pltpu.make_async_remote_copy(
            ysend.at[iy], yrecv.at[iy], y_sem.at[0, iy], y_sem.at[1, iy],
            device_id={"gy": around["gy"][signs[iy]]}, device_id_type=MESH,
        )

    def yz_copy(iy, iz):
        return pltpu.make_async_remote_copy(
            ysend.at[iy, pl.ds(18 - (2 - iz) * EDGE, EDGE)], yzrecv.at[iy, iz],
            yz_sem.at[0, iy, iz], yz_sem.at[1, iy, iz],
            device_id={"gy": around["gy"][signs[iy]], "gz": around["gz"][signs[iz]]}, device_id_type=MESH,
        )

    def slabs(fast):
        for members in (TILTED, FLAT):
            for ix, sign in enumerate(signs):
                for member in members[sign]:
                    if (abs(SPEEDS[member][0]) == 3) == fast:
                        x_copy(ix, member).start()

    def meet(own, count):
        @pl.when(core == own)
        def _():
            pl.semaphore_wait(barrier, count)
            tell(pair_sem, gz=partner)

        @pl.when(core != own)
        def _():
            pl.semaphore_wait(pair_sem, 1)

    def meet_x():
        meet(0, 7)

    def meet_y():
        meet(1, 5)

    def corners(iy):
        pl.semaphore_wait(ready_sem.at[iy], 1)
        for number, (sx, sy) in enumerate(CORNERS):
            if sy == signs[iy]:
                d_copy(number).start()
                for iz in range(2):
                    dz_copy(number, iz).start()

    def edges(iy):
        for iz in range(2):
            yz_copy(iy, iz).start()

    last = lax.axis_index("gy") == lax.axis_size("gy") - 1
    not_last = jnp.logical_not(last)
    x_first = jnp.logical_and(not_last, lax.axis_index("gx") > 0)
    rate_load.wait()
    lax.fori_loop(0, 2, lambda turn, carry: collide_layer(nx - 1 - turn, carry), 0)
    lax.fori_loop(0, 2, collide_layer, 0)
    for number, (sx, sy) in enumerate(CORNERS):
        for place, (member, layer, row) in enumerate(corner_rows(sx, sy)):
            x = nx - abs(SPEEDS[member][0]) + layer if sx > 0 else layer
            dsend[number, pl.ds(place, 1), :] = p_ref[member, x, pl.ds(leaving_row(member, row, ny), 1), :]

    @pl.when(x_first)
    def _():
        meet_x()
        slabs(False)

    @pl.when(last)
    def _():
        meet_y()
        corners(0)

    lax.fori_loop(2, nx - 2, collide_layer, 0)

    @pl.when(x_first)
    def _():
        slabs(True)

    for iy, sign in enumerate(signs):
        for member, offset in YS[sign].items():
            for row in range(abs(SPEEDS[member][1])):
                ysend[iy, offset + row] = read_rows(p_ref, member, leaving_row(member, row, ny))

    @pl.when(not_last)
    def _():
        meet_y()

    for iy in range(2):
        y_copy(iy).start()

    @pl.when(last)
    def _():
        edges(0)

    @pl.when(jnp.logical_not(x_first))
    def _():
        meet_x()

    for sign in signs:
        tell(plane_sem, gz=around["gz"][sign])
    for index in range(2):
        for pair in range(nx // 2):
            fold_z(index, pair)
    for index in range(2):
        z_copy(index).start()
    pl.semaphore_wait(plane_sem, 2)
    for iy, sign in enumerate(signs):
        tell(ready_sem.at[1 - iy], gy=around["gy"][sign])
    for ix in range(2):
        for iz in range(2):
            xz_copy(ix, iz).start()

    @pl.when(jnp.logical_not(x_first))
    def _():
        slabs(False)
        slabs(True)

    @pl.when(not_last)
    def _():
        corners(0)
        edges(0)

    corners(1)
    edges(1)

    def merge_z(index, wanted):
        for pair in range(nx // 2):
            columns = zrecv[index, pair]
            for half in range(2):
                for block in range(blocks):
                    for member in ZS[signs[index]]:
                        x = 2 * pair + half
                        if wanted(member, x):
                            unfold(columns, p_ref.at[member, x], member, half, block, row_of(member, block))

    def travels(member, x):
        cx = SPEEDS[member][0]
        return x >= nx - cx if cx > 0 else x < -cx

    for index in range(2):
        z_copy(index).wait_recv()
        merge_z(index, lambda member, x: not travels(member, x))
    for members in (TILTED, FLAT):
        for ix, sign in enumerate(signs):
            for member in members[sign]:
                x_copy(ix, member).wait_send()
    for index in range(2):
        merge_z(index, travels)
    for iy, sign in enumerate(signs):
        y_copy(iy).wait_recv()
        for iz in range(2):
            yz_copy(iy, iz).wait_recv()
        for member, offset in YS[sign].items():
            cz = SPEEDS[member][2]
            for row in range(abs(SPEEDS[member][1])):
                value = yrecv[iy, offset + row]
                if cz != 0:
                    iz = 0 if cz > 0 else 1
                    edge = yzrecv[iy, iz, offset + row - 18 + (2 - iz) * EDGE]
                    value = jnp.where(enters(signs[iz], abs(cz)), edge, value)
                write_rows(p_ref, member, entering_row(member, row, ny), value)
    for ix, sign in enumerate(signs):
        for iz in range(2):
            xz_copy(ix, iz).wait_recv()
        for member in TILTED[sign]:
            x_copy(ix, member).wait_recv()
            reach, iz = abs(SPEEDS[member][0]), 0 if SPEEDS[member][2] > 0 else 1
            for layer in range(reach):
                half = 2 - reach + layer if sign > 0 else layer
                for block in range(blocks):
                    target = halo[ix].at[XS[sign][member] + layer]
                    unfold(xzrecv[ix, iz], target, member, half, block, row_of(member, block))
    for ix, sign in enumerate(signs):
        for member in FLAT[sign]:
            x_copy(ix, member).wait_recv()
    for number, (sx, sy) in enumerate(CORNERS):
        ix = 0 if sx > 0 else 1
        d_copy(number).wait_recv()
        for iz in range(2):
            dz_copy(number, iz).wait_recv()
        for place, (member, layer, row) in enumerate(corner_rows(sx, sy)):
            cz = SPEEDS[member][2]
            value = drecv[number, pl.ds(place, 1), :]
            if cz != 0:
                iz = 0 if cz > 0 else 1
                mask = enters(signs[iz], abs(cz))[:1]
                value = jnp.where(mask, dzrecv[number, iz, pl.ds(place, 1), :], value)
            halo[ix][XS[sx][member] + layer, pl.ds(entering_row(member, row, ny), 1), :] = value
    for index in range(2):
        z_copy(index).wait_send()
        y_copy(index).wait_send()
        for iz in range(2):
            xz_copy(index, iz).wait_send()
            yz_copy(index, iz).wait_send()
    for number in range(4):
        d_copy(number).wait_send()
        for iz in range(2):
            dz_copy(number, iz).wait_send()


def emit_kernel(sizes, p_ref, up_ref, down_ref, o_hbm, sem):
    nx, ny, nz = sizes
    copies = []
    for member in range(Q):
        cx = SPEEDS[member][0]
        rows = pl.ds(final_row(member), ny)
        if cx > 0:
            pieces = [
                (p_ref.at[member, pl.ds(0, nx - cx), rows, :], o_hbm.at[member, pl.ds(cx, nx - cx)]),
                (up_ref.at[pl.ds(XS[1][member], cx), rows, :], o_hbm.at[member, pl.ds(0, cx)]),
            ]
        elif cx < 0:
            pieces = [
                (p_ref.at[member, pl.ds(-cx, nx + cx), rows, :], o_hbm.at[member, pl.ds(0, nx + cx)]),
                (down_ref.at[pl.ds(XS[-1][member], -cx), rows, :], o_hbm.at[member, pl.ds(nx + cx, -cx)]),
            ]
        else:
            pieces = [(p_ref.at[member, :, rows, :], o_hbm.at[member])]
        for source, target in pieces:
            copies.append(pltpu.make_async_copy(source, target, sem.at[len(copies)]))
    for copy in copies:
        copy.start()
    for copy in copies:
        copy.wait()


def per_device(populations, relax):
    sizes = populations.shape[1:]
    nx, ny, nz = sizes
    blocks = ny // 8
    vmem = pl.BlockSpec(memory_space=pltpu.VMEM)
    hbm = pl.BlockSpec(memory_space=pltpu.HBM)
    dma = pltpu.SemaphoreType.DMA
    shifted, up, down = pl.pallas_call(
        functools.partial(exchange_kernel, sizes),
        out_shape=(
            jax.ShapeDtypeStruct((Q, nx, ROWS, nz), F32),
            jax.ShapeDtypeStruct((18, ROWS, nz), F32),
            jax.ShapeDtypeStruct((18, ROWS, nz), F32),
        ),
        in_specs=[hbm, hbm],
        out_specs=(vmem, vmem, vmem),
        scratch_shapes=[
            pltpu.VMEM((Q, nx, ny, nz), F32),
            pltpu.VMEM((nx, ny, nz), F32),
            pltpu.VMEM((2, nx, blocks, 8, nz), F32),
            pltpu.VMEM((2, nx // 2, 8, nz), F32),
            pltpu.VMEM((2, nx // 2, 8, nz), F32),
            pltpu.VMEM((2, 2, 8, nz), F32),
            pltpu.VMEM((2, 18, nx, nz), F32),
            pltpu.VMEM((2, 18, nx, nz), F32),
            pltpu.VMEM((2, 2, EDGE, nx, nz), F32),
            pltpu.VMEM((4, 8, nz), F32),
            pltpu.VMEM((4, 8, nz), F32),
            pltpu.VMEM((4, 2, 8, nz), F32),
            dma((nx + 1,)),
            dma((2, 2)),
            dma((2, 2, 2)),
            dma((2, 2)),
            dma((2, 2, 2)),
            dma((2, 4)),
            dma((2, 4, 2)),
            dma((2, 2, 11)),
            pltpu.SemaphoreType.REGULAR,
            pltpu.SemaphoreType.REGULAR,
            pltpu.SemaphoreType.REGULAR((2,)),
        ],
        compiler_params=pltpu.CompilerParams(
            collective_id=0, has_side_effects=True, vmem_limit_bytes=24 * 1024 * 1024
        ),
        name="collide_exchange",
    )(*(pltpu.with_memory_space_constraint(array, pltpu.HBM) for array in (populations, relax)))
    return pl.pallas_call(
        functools.partial(emit_kernel, sizes),
        out_shape=jax.ShapeDtypeStruct(populations.shape, F32),
        in_specs=[vmem, vmem, vmem],
        out_specs=hbm,
        scratch_shapes=[dma((61,))],
        compiler_params=pltpu.CompilerParams(vmem_limit_bytes=24 * 1024 * 1024),
        name="emit",
    )(shifted, up, down)


def solution(mesh):
    return jax.shard_map(
        per_device,
        mesh=mesh,
        in_specs=(P(None, "gx", "gy", "gz"), P("gx", "gy", "gz")),
        out_specs=P(None, "gx", "gy", "gz"),
        check_vma=False,
    )
```

```python
import functools

import jax
import jax.numpy as jnp
from jax import lax
from jax.experimental import pallas as pl
from jax.experimental.pallas import tpu as pltpu
from jax.sharding import PartitionSpec as P

MESH = pl.DeviceIdType.MESH
F32 = jnp.float32


def lattice():
    speeds = [(0, 0, 0)]
    weights = [1.0 / 12.0]
    for axis in range(3):
        for sign in (1, -1):
            vector = [0, 0, 0]
            vector[axis] = sign
            speeds.append(tuple(vector))
            weights.append(1.0 / 12.0)
    for first in (1, -1):
        for second in (1, -1):
            for third in (1, -1):
                speeds.append((first, second, third))
                weights.append(1.0 / 27.0)
    for axis in range(3):
        for sign in (2, -2):
            vector = [0, 0, 0]
            vector[axis] = sign
            speeds.append(tuple(vector))
            weights.append(2.0 / 135.0)
    for couple in ((0, 1), (0, 2), (1, 2)):
        for first in (2, -2):
            for second in (2, -2):
                vector = [0, 0, 0]
                vector[couple[0]] = first
                vector[couple[1]] = second
                speeds.append(tuple(vector))
                weights.append(1.0 / 432.0)
    for axis in range(3):
        for sign in (3, -3):
            vector = [0, 0, 0]
            vector[axis] = sign
            speeds.append(tuple(vector))
            weights.append(1.0 / 1620.0)
    return speeds, weights


SPEEDS, WEIGHTS = lattice()
Q = 39
INDEX = {vector: member for member, vector in enumerate(SPEEDS)}
ROWS = 32


def slots(axis, sign):
    table, offset = {}, 0
    for third in (0, 1, -1):
        for member in range(Q):
            speed = SPEEDS[member][axis] * sign
            cz = SPEEDS[member][2] if axis < 2 else 0
            if speed > 0 and (cz > 0) - (cz < 0) == third:
                table[member] = offset
                offset += speed
    return table


XS = {sign: slots(0, sign) for sign in (1, -1)}
YS = {sign: slots(1, sign) for sign in (1, -1)}
ZS = {sign: slots(2, sign) for sign in (1, -1)}
FLAT = {sign: [m for m in XS[sign] if SPEEDS[m][2] == 0] for sign in (1, -1)}
TILTED = {sign: [m for m in XS[sign] if SPEEDS[m][2] != 0] for sign in (1, -1)}
EDGE = 4
CORNERS = [(1, 1), (1, -1), (-1, 1), (-1, -1)]
SHELLS = {0.0: "0", 1.0: "1", 3.0: "c", 4.0: "2", 8.0: "e", 9.0: "3"}


def square(member):
    return float(sum(value * value for value in SPEEDS[member]))


def final_row(member):
    return 8 if SPEEDS[member][1] < 0 else 0


def corner_rows(sx, sy):
    rows = []
    for member in range(Q):
        cx, cy = SPEEDS[member][0] * sx, SPEEDS[member][1] * sy
        if cx > 0 and cy > 0:
            rows += [(member, layer, row) for layer in range(cx) for row in range(cy)]
    return rows


def leaving_row(member, row, ny):
    cy = SPEEDS[member][1]
    return ny + row if cy > 0 else 8 + cy + row


def entering_row(member, row, ny):
    cy = SPEEDS[member][1]
    return row if cy > 0 else 8 + ny + cy + row


def strided(ref, member, row):
    count, layers, rows, lanes = ref.shape
    return ref.reshape(count * layers * rows, lanes), pl.ds(member * layers * rows + row, layers, stride=rows)


def read_rows(ref, member, row):
    flat, where = strided(ref, member, row)
    return flat[where, :]


def write_rows(ref, member, row, value):
    flat, where = strided(ref, member, row)
    flat[where, :] = value


def collide(load, rate, store):
    weight = {shell: WEIGHTS[m] for m in range(Q) for shell in [SHELLS[square(m)]]}
    total = {}
    odd = {}
    for member in range(Q):
        vector = SPEEDS[member]
        shell = SHELLS[square(member)]
        opposite = INDEX[tuple(-value for value in vector)]
        if member == opposite:
            total[shell] = load(member)
        elif member < opposite:
            one, other = load(member), load(opposite)
            both = one + other
            total[shell] = total[shell] + both if shell in total else both
            odd[member] = one - other
    density = sum(weight[shell] * total[shell] for shell in total)
    energy = sum(weight[SHELLS[v]] * v * total[SHELLS[v]] for v in (1.0, 3.0, 4.0, 8.0, 9.0))
    inverse = 1.0 / density
    drift = []
    for axis in range(3):
        parts = {}
        for member, value in odd.items():
            speed = SPEEDS[member][axis]
            if speed == 0:
                continue
            key = (SHELLS[square(member)], abs(speed))
            if key in parts:
                parts[key] = parts[key] + value if speed > 0 else parts[key] - value
            else:
                parts[key] = value if speed > 0 else -value
        flux = sum((weight[shell] * speed * 1.5) * value for (shell, speed), value in parts.items())
        drift.append(flux * inverse)
    w = drift
    ww = [value * value for value in w]
    norm = (ww[0] + ww[1] + ww[2]) * (4.0 / 9.0)
    t = (energy * inverse - norm) * 0.5 - 1.0
    b = 1.5 * norm
    scale = rate * density
    keep = 1.0 - rate
    tb = t * b
    t2 = t * t
    p0 = scale * (1.0 - 0.5 * b + 0.125 * b * b - 1.5 * t + 1.25 * tb + 1.875 * t2)
    p1 = scale * (0.5 * t - 0.25 * tb - 1.25 * t2)
    p2 = scale * (0.125 * t2)
    st = scale * t
    b0 = scale * (0.5 - 0.25 * b) - 1.75 * st
    c0 = scale * (1.0 - 0.5 * b) - 2.5 * st
    quart = {k: (k**4 / 24.0) * scale for k in (1, 2, 3)}
    cubic = {k: (k**3 / 6.0) * scale for k in (1, 2, 3)}
    reach = {"1": 1, "c": 1, "2": 2, "e": 2, "3": 3}
    coefficients = {}
    for value, shell in SHELLS.items():
        s = 1.5 * value
        even = p0 + s * p1 + (s * s) * p2 if s else p0
        if s:
            k = reach[shell]
            coefficients[shell] = (
                even,
                (k * k) * b0 + (k * k * s * 0.25) * st,
                k * c0 + (k * s * 0.5) * st,
                quart[k],
                cubic[k],
            )
        else:
            coefficients[shell] = even
    for member in range(Q):
        vector = SPEEDS[member]
        shell = SHELLS[square(member)]
        opposite = INDEX[tuple(-value for value in vector)]
        if member == opposite:
            store(member, keep * load(member) + coefficients[shell])
        elif member < opposite:
            k = reach[shell]
            q, q2 = None, None
            axes = [axis for axis in range(3) if vector[axis] != 0]
            if len(axes) == 1:
                q, q2 = w[axes[0]], ww[axes[0]]
            else:
                q = w[axes[0]]
                for axis in axes[1:]:
                    q = q + w[axis] if vector[axis] > 0 else q - w[axis]
                q2 = q * q
            e0, e2, o1, e4, o3 = coefficients[shell]
            even = e0 + q2 * (e2 + q2 * e4)
            uneven = q * (o1 + q2 * o3)
            store(member, keep * load(member) + (even + uneven))
            store(opposite, keep * load(opposite) + (even - uneven))


def exchange_kernel(
    sizes, g_hbm, r_hbm, p_ref, up_ref, down_ref,
    g, rate, zraw, zsend, zrecv, xzrecv, ysend, yrecv, yzrecv, dsend, drecv, dzrecv,
    load_sem, z_sem, xz_sem, y_sem, yz_sem, d_sem, dz_sem, x_sem, pair_sem, plane_sem, ready_sem,
):
    nx, ny, nz = sizes
    blocks = ny // 8
    signs = (1, -1)
    around = {}
    for axis in ("gx", "gy", "gz"):
        me, count = lax.axis_index(axis), lax.axis_size(axis)
        around[axis] = {1: lax.rem(me + 1, count), -1: lax.rem(me + count - 1, count)}

    def layer_load(x):
        return pltpu.make_async_copy(g_hbm.at[:, pl.ds(x, 1)], g.at[:, pl.ds(x, 1)], load_sem.at[x])

    rate_load = pltpu.make_async_copy(r_hbm, rate, load_sem.at[nx])
    rate_load.start()
    for x in [nx - 1, nx - 2, 0, 1] + list(range(2, nx - 2)):
        layer_load(x).start()

    barrier = pltpu.get_barrier_semaphore()
    gz = lax.axis_index("gz")
    core = lax.rem(gz, 2)
    chip = gz - core
    other_chip = lax.rem(chip + 2, lax.axis_size("gz"))
    partner = chip + 1 - core

    def tell(semaphore, **device):
        pl.semaphore_signal(semaphore, inc=1, device_id=device, device_id_type=MESH)

    for sign in signs:
        tell(barrier, gx=around["gx"][sign], gz=chip)
        tell(barrier, gy=around["gy"][sign], gz=chip + 1)
    tell(barrier, gz=other_chip)

    tell(barrier, gz=partner)

    lane = lax.broadcasted_iota(jnp.int32, (8, nz), 1)
    pack_masks = {offset: lane >= offset for offset in sorted(set(ZS[1].values())) if offset}

    def row_of(member, block):
        return pl.ds(final_row(member) + SPEEDS[member][1] + 8 * block, 8)

    def collide_block(x, block):
        pieces = {1: {}, -1: {}}

        def load(member):
            return g[member, x, pl.ds(8 * block, 8), :]

        def store(member, value):
            cz = SPEEDS[member][2]
            if cz != 0:
                p_ref[member, x, row_of(member, block), :] = pltpu.roll(value, cz % nz, 1)
                sign = 1 if cz > 0 else -1
                place = ZS[sign][member]
                shift = (place + max(cz, 0)) % nz
                pieces[sign][place] = pltpu.roll(value, shift, 1) if shift else value
            else:
                p_ref[member, x, row_of(member, block), :] = value

        collide(load, rate[x, pl.ds(8 * block, 8), :], store)
        for index, sign in enumerate(signs):
            packed = None
            for place in sorted(pieces[sign]):
                packed = pieces[sign][place] if packed is None else jnp.where(pack_masks[place], pieces[sign][place], packed)
            zraw[index, x, block] = packed

    def collide_layer(x, carry):
        layer_load(x).wait()
        for block in range(blocks):
            collide_block(x, block)
        return carry

    def column(half, block, offset):
        return 18 * (half * blocks + block) + offset

    def fold_z(index, pair):
        packed = None
        for half in range(2):
            for block in range(blocks):
                place = column(half, block, 0)
                value = zraw[index, 2 * pair + half, block]
                packed = value if packed is None else jnp.where(lane >= place, pltpu.roll(value, place, 1), packed)
        zsend[index, pair] = packed

    def enters(sign, reach):
        return lane < reach if sign > 0 else lane >= nz - reach

    def unfold(columns, target, member, half, block, rows):
        cz = SPEEDS[member][2]
        sign, reach = (1, cz) if cz > 0 else (-1, -cz)
        place = column(half, block, ZS[sign][member])
        shift = ((0 if sign > 0 else nz - reach) - place) % nz
        value = pltpu.roll(columns, shift, 1) if shift else columns
        pltpu.store(target.at[rows, :], value, mask=enters(sign, reach))

    def z_copy(index):
        return pltpu.make_async_remote_copy(
            zsend.at[index], zrecv.at[index], z_sem.at[0, index], z_sem.at[1, index],
            device_id={"gz": around["gz"][signs[index]]}, device_id_type=MESH,
        )

    def xz_copy(ix, iz):
        pair = nx // 2 - 1 if ix == 0 else 0
        return pltpu.make_async_remote_copy(
            zsend.at[iz, pair], xzrecv.at[ix, iz], xz_sem.at[0, ix, iz], xz_sem.at[1, ix, iz],
            device_id={"gx": around["gx"][signs[ix]], "gz": around["gz"][signs[iz]]}, device_id_type=MESH,
        )

    halo = (up_ref, down_ref)

    def x_copy(ix, member):
        sign, reach = signs[ix], abs(SPEEDS[member][0])
        rows = pl.ds(final_row(member), ny)
        layers = pl.ds(nx - reach, reach) if sign > 0 else pl.ds(0, reach)
        place = list(XS[sign]).index(member)
        return pltpu.make_async_remote_copy(
            p_ref.at[member, layers, rows, :], halo[ix].at[pl.ds(XS[sign][member], reach), rows, :],
            x_sem.at[0, ix, place], x_sem.at[1, ix, place],
            device_id={"gx": around["gx"][sign]}, device_id_type=MESH,
        )

    def d_copy(number):
        sx, sy = CORNERS[number]
        return pltpu.make_async_remote_copy(
            dsend.at[number], drecv.at[number], d_sem.at[0, number], d_sem.at[1, number],
            device_id={"gx": around["gx"][sx], "gy": around["gy"][sy]}, device_id_type=MESH,
        )

    def dz_copy(number, iz):
        sx, sy = CORNERS[number]
        return pltpu.make_async_remote_copy(
            dsend.at[number], dzrecv.at[number, iz], dz_sem.at[0, number, iz], dz_sem.at[1, number, iz],
            device_id={"gx": around["gx"][sx], "gy": around["gy"][sy], "gz": around["gz"][signs[iz]]},
            device_id_type=MESH,
        )

    def y_copy(iy):
        return pltpu.make_async_remote_copy(
            ysend.at[iy], yrecv.at[iy], y_sem.at[0, iy], y_sem.at[1, iy],
            device_id={"gy": around["gy"][signs[iy]]}, device_id_type=MESH,
        )

    def yz_copy(iy, iz):
        return pltpu.make_async_remote_copy(
            ysend.at[iy, pl.ds(18 - (2 - iz) * EDGE, EDGE)], yzrecv.at[iy, iz],
            yz_sem.at[0, iy, iz], yz_sem.at[1, iy, iz],
            device_id={"gy": around["gy"][signs[iy]], "gz": around["gz"][signs[iz]]}, device_id_type=MESH,
        )

    def slabs(fast):
        for members in (TILTED, FLAT):
            for ix, sign in enumerate(signs):
                for member in members[sign]:
                    if (abs(SPEEDS[member][0]) == 3) == fast:
                        x_copy(ix, member).start()

    def meet(own, count):
        @pl.when(core == own)
        def _():
            pl.semaphore_wait(barrier, count)
            tell(pair_sem, gz=partner)

        @pl.when(core != own)
        def _():
            pl.semaphore_wait(pair_sem, 1)

    def meet_x():
        meet(0, 7)

    def meet_y():
        meet(1, 5)

    def corners(iy):
        pl.semaphore_wait(ready_sem.at[iy], 1)
        for number, (sx, sy) in enumerate(CORNERS):
            if sy == signs[iy]:
                d_copy(number).start()
                for iz in range(2):
                    dz_copy(number, iz).start()

    def edges(iy):
        for iz in range(2):
            yz_copy(iy, iz).start()

    last = lax.axis_index("gy") == lax.axis_size("gy") - 1
    not_last = jnp.logical_not(last)
    first = lax.axis_index("gy") == 0
    x_first = lax.axis_index("gx") > 0
    rate_load.wait()
    lax.fori_loop(0, 2, lambda turn, carry: collide_layer(nx - 1 - turn, carry), 0)
    lax.fori_loop(0, 2, collide_layer, 0)
    for number, (sx, sy) in enumerate(CORNERS):
        for place, (member, layer, row) in enumerate(corner_rows(sx, sy)):
            x = nx - abs(SPEEDS[member][0]) + layer if sx > 0 else layer
            dsend[number, pl.ds(place, 1), :] = p_ref[member, x, pl.ds(leaving_row(member, row, ny), 1), :]

    @pl.when(last)
    def _():
        meet_y()
        corners(0)

    @pl.when(x_first)
    def _():
        meet_x()
        slabs(False)

    lax.fori_loop(2, nx - 2, collide_layer, 0)

    @pl.when(x_first)
    def _():
        slabs(True)

    for iy, sign in enumerate(signs):
        for member, offset in YS[sign].items():
            for row in range(abs(SPEEDS[member][1])):
                ysend[iy, offset + row] = read_rows(p_ref, member, leaving_row(member, row, ny))

    @pl.when(not_last)
    def _():
        meet_y()

    for iy in range(2):
        y_copy(iy).start()

    @pl.when(last)
    def _():
        edges(0)

    @pl.when(jnp.logical_not(x_first))
    def _():
        meet_x()

    for sign in signs:
        tell(plane_sem, gz=around["gz"][sign])
    for index in range(2):
        for pair in range(nx // 2):
            fold_z(index, pair)
    for index in range(2):
        z_copy(index).start()
    pl.semaphore_wait(plane_sem, 2)
    for iy, sign in enumerate(signs):
        tell(ready_sem.at[1 - iy], gy=around["gy"][sign])
    for ix in range(2):
        for iz in range(2):
            xz_copy(ix, iz).start()

    @pl.when(jnp.logical_not(x_first))
    def _():
        slabs(False)
        slabs(True)

    @pl.when(not_last)
    def _():
        corners(0)
        edges(0)

    def finish_edges():
        corners(1)
        edges(1)

    pl.when(jnp.logical_not(first))(finish_edges)

    def merge_z(index, wanted):
        for pair in range(nx // 2):
            columns = zrecv[index, pair]
            for half in range(2):
                for block in range(blocks):
                    for member in ZS[signs[index]]:
                        x = 2 * pair + half
                        if wanted(member, x):
                            unfold(columns, p_ref.at[member, x], member, half, block, row_of(member, block))

    def travels(member, x):
        cx = SPEEDS[member][0]
        return x >= nx - cx if cx > 0 else x < -cx

    for index in range(2):
        z_copy(index).wait_recv()
        merge_z(index, lambda member, x: not travels(member, x))
    pl.when(first)(finish_edges)
    for members in (TILTED, FLAT):
        for ix, sign in enumerate(signs):
            for member in members[sign]:
                x_copy(ix, member).wait_send()
    for index in range(2):
        merge_z(index, travels)
    for iy, sign in enumerate(signs):
        y_copy(iy).wait_recv()
        for iz in range(2):
            yz_copy(iy, iz).wait_recv()
        for member, offset in YS[sign].items():
            cz = SPEEDS[member][2]
            for row in range(abs(SPEEDS[member][1])):
                value = yrecv[iy, offset + row]
                if cz != 0:
                    iz = 0 if cz > 0 else 1
                    edge = yzrecv[iy, iz, offset + row - 18 + (2 - iz) * EDGE]
                    value = jnp.where(enters(signs[iz], abs(cz)), edge, value)
                write_rows(p_ref, member, entering_row(member, row, ny), value)
    for ix, sign in enumerate(signs):
        for iz in range(2):
            xz_copy(ix, iz).wait_recv()
        for member in TILTED[sign]:
            x_copy(ix, member).wait_recv()
            reach, iz = abs(SPEEDS[member][0]), 0 if SPEEDS[member][2] > 0 else 1
            for layer in range(reach):
                half = 2 - reach + layer if sign > 0 else layer
                for block in range(blocks):
                    target = halo[ix].at[XS[sign][member] + layer]
                    unfold(xzrecv[ix, iz], target, member, half, block, row_of(member, block))
    for ix, sign in enumerate(signs):
        for member in FLAT[sign]:
            x_copy(ix, member).wait_recv()
    for number, (sx, sy) in enumerate(CORNERS):
        ix = 0 if sx > 0 else 1
        d_copy(number).wait_recv()
        for iz in range(2):
            dz_copy(number, iz).wait_recv()
        for place, (member, layer, row) in enumerate(corner_rows(sx, sy)):
            cz = SPEEDS[member][2]
            value = drecv[number, pl.ds(place, 1), :]
            if cz != 0:
                iz = 0 if cz > 0 else 1
                mask = enters(signs[iz], abs(cz))[:1]
                value = jnp.where(mask, dzrecv[number, iz, pl.ds(place, 1), :], value)
            halo[ix][XS[sx][member] + layer, pl.ds(entering_row(member, row, ny), 1), :] = value
    for index in range(2):
        z_copy(index).wait_send()
        y_copy(index).wait_send()
        for iz in range(2):
            xz_copy(index, iz).wait_send()
            yz_copy(index, iz).wait_send()
    for number in range(4):
        d_copy(number).wait_send()
        for iz in range(2):
            dz_copy(number, iz).wait_send()


def emit_kernel(sizes, p_ref, up_ref, down_ref, o_hbm, sem):
    nx, ny, nz = sizes
    copies = []
    for member in range(Q):
        cx = SPEEDS[member][0]
        rows = pl.ds(final_row(member), ny)
        if cx > 0:
            pieces = [
                (p_ref.at[member, pl.ds(0, nx - cx), rows, :], o_hbm.at[member, pl.ds(cx, nx - cx)]),
                (up_ref.at[pl.ds(XS[1][member], cx), rows, :], o_hbm.at[member, pl.ds(0, cx)]),
            ]
        elif cx < 0:
            pieces = [
                (p_ref.at[member, pl.ds(-cx, nx + cx), rows, :], o_hbm.at[member, pl.ds(0, nx + cx)]),
                (down_ref.at[pl.ds(XS[-1][member], -cx), rows, :], o_hbm.at[member, pl.ds(nx + cx, -cx)]),
            ]
        else:
            pieces = [(p_ref.at[member, :, rows, :], o_hbm.at[member])]
        for source, target in pieces:
            copies.append(pltpu.make_async_copy(source, target, sem.at[len(copies)]))
    for copy in copies:
        copy.start()
    for copy in copies:
        copy.wait()


def per_device(populations, relax):
    sizes = populations.shape[1:]
    nx, ny, nz = sizes
    blocks = ny // 8
    vmem = pl.BlockSpec(memory_space=pltpu.VMEM)
    hbm = pl.BlockSpec(memory_space=pltpu.HBM)
    dma = pltpu.SemaphoreType.DMA
    shifted, up, down = pl.pallas_call(
        functools.partial(exchange_kernel, sizes),
        out_shape=(
            jax.ShapeDtypeStruct((Q, nx, ROWS, nz), F32),
            jax.ShapeDtypeStruct((18, ROWS, nz), F32),
            jax.ShapeDtypeStruct((18, ROWS, nz), F32),
        ),
        in_specs=[hbm, hbm],
        out_specs=(vmem, vmem, vmem),
        scratch_shapes=[
            pltpu.VMEM((Q, nx, ny, nz), F32),
            pltpu.VMEM((nx, ny, nz), F32),
            pltpu.VMEM((2, nx, blocks, 8, nz), F32),
            pltpu.VMEM((2, nx // 2, 8, nz), F32),
            pltpu.VMEM((2, nx // 2, 8, nz), F32),
            pltpu.VMEM((2, 2, 8, nz), F32),
            pltpu.VMEM((2, 18, nx, nz), F32),
            pltpu.VMEM((2, 18, nx, nz), F32),
            pltpu.VMEM((2, 2, EDGE, nx, nz), F32),
            pltpu.VMEM((4, 8, nz), F32),
            pltpu.VMEM((4, 8, nz), F32),
            pltpu.VMEM((4, 2, 8, nz), F32),
            dma((nx + 1,)),
            dma((2, 2)),
            dma((2, 2, 2)),
            dma((2, 2)),
            dma((2, 2, 2)),
            dma((2, 4)),
            dma((2, 4, 2)),
            dma((2, 2, 11)),
            pltpu.SemaphoreType.REGULAR,
            pltpu.SemaphoreType.REGULAR,
            pltpu.SemaphoreType.REGULAR((2,)),
        ],
        compiler_params=pltpu.CompilerParams(
            collective_id=0, has_side_effects=True, vmem_limit_bytes=24 * 1024 * 1024
        ),
        name="collide_exchange",
    )(*(pltpu.with_memory_space_constraint(array, pltpu.HBM) for array in (populations, relax)))
    return pl.pallas_call(
        functools.partial(emit_kernel, sizes),
        out_shape=jax.ShapeDtypeStruct(populations.shape, F32),
        in_specs=[vmem, vmem, vmem],
        out_specs=hbm,
        scratch_shapes=[dma((61,))],
        compiler_params=pltpu.CompilerParams(vmem_limit_bytes=24 * 1024 * 1024),
        name="emit",
    )(shifted, up, down)


def solution(mesh):
    return jax.shard_map(
        per_device,
        mesh=mesh,
        in_specs=(P(None, "gx", "gy", "gz"), P("gx", "gy", "gz")),
        out_specs=P(None, "gx", "gy", "gz"),
        check_vma=False,
    )
```

```python
import functools

import jax
import jax.numpy as jnp
from jax import lax
from jax.experimental import pallas as pl
from jax.experimental.pallas import tpu as pltpu
from jax.sharding import PartitionSpec as P

MESH = pl.DeviceIdType.MESH
F32 = jnp.float32


def lattice():
    speeds = [(0, 0, 0)]
    weights = [1.0 / 12.0]
    for axis in range(3):
        for sign in (1, -1):
            vector = [0, 0, 0]
            vector[axis] = sign
            speeds.append(tuple(vector))
            weights.append(1.0 / 12.0)
    for first in (1, -1):
        for second in (1, -1):
            for third in (1, -1):
                speeds.append((first, second, third))
                weights.append(1.0 / 27.0)
    for axis in range(3):
        for sign in (2, -2):
            vector = [0, 0, 0]
            vector[axis] = sign
            speeds.append(tuple(vector))
            weights.append(2.0 / 135.0)
    for couple in ((0, 1), (0, 2), (1, 2)):
        for first in (2, -2):
            for second in (2, -2):
                vector = [0, 0, 0]
                vector[couple[0]] = first
                vector[couple[1]] = second
                speeds.append(tuple(vector))
                weights.append(1.0 / 432.0)
    for axis in range(3):
        for sign in (3, -3):
            vector = [0, 0, 0]
            vector[axis] = sign
            speeds.append(tuple(vector))
            weights.append(1.0 / 1620.0)
    return speeds, weights


SPEEDS, WEIGHTS = lattice()
Q = 39
INDEX = {vector: member for member, vector in enumerate(SPEEDS)}
ROWS = 32


def slots(axis, sign):
    table, offset = {}, 0
    for third in (0, 1, -1):
        for member in range(Q):
            speed = SPEEDS[member][axis] * sign
            cz = SPEEDS[member][2] if axis < 2 else 0
            if speed > 0 and (cz > 0) - (cz < 0) == third:
                table[member] = offset
                offset += speed
    return table


XS = {sign: slots(0, sign) for sign in (1, -1)}
YS = {sign: slots(1, sign) for sign in (1, -1)}
ZS = {sign: slots(2, sign) for sign in (1, -1)}
FLAT = {sign: [m for m in XS[sign] if SPEEDS[m][2] == 0] for sign in (1, -1)}
TILTED = {sign: [m for m in XS[sign] if SPEEDS[m][2] != 0] for sign in (1, -1)}
EDGE = 4
CORNERS = [(1, 1), (1, -1), (-1, 1), (-1, -1)]
SHELLS = {0.0: "0", 1.0: "1", 3.0: "c", 4.0: "2", 8.0: "e", 9.0: "3"}


def square(member):
    return float(sum(value * value for value in SPEEDS[member]))


def final_row(member):
    return 8 if SPEEDS[member][1] < 0 else 0


def corner_rows(sx, sy):
    rows = []
    for member in range(Q):
        cx, cy = SPEEDS[member][0] * sx, SPEEDS[member][1] * sy
        if cx > 0 and cy > 0:
            rows += [(member, layer, row) for layer in range(cx) for row in range(cy)]
    return rows


def leaving_row(member, row, ny):
    cy = SPEEDS[member][1]
    return ny + row if cy > 0 else 8 + cy + row


def entering_row(member, row, ny):
    cy = SPEEDS[member][1]
    return row if cy > 0 else 8 + ny + cy + row


def strided(ref, member, row):
    count, layers, rows, lanes = ref.shape
    return ref.reshape(count * layers * rows, lanes), pl.ds(member * layers * rows + row, layers, stride=rows)


def read_rows(ref, member, row):
    flat, where = strided(ref, member, row)
    return flat[where, :]


def write_rows(ref, member, row, value):
    flat, where = strided(ref, member, row)
    flat[where, :] = value


def collide(load, rate, store):
    weight = {shell: WEIGHTS[m] for m in range(Q) for shell in [SHELLS[square(m)]]}
    total = {}
    odd = {}
    for member in range(Q):
        vector = SPEEDS[member]
        shell = SHELLS[square(member)]
        opposite = INDEX[tuple(-value for value in vector)]
        if member == opposite:
            total[shell] = load(member)
        elif member < opposite:
            one, other = load(member), load(opposite)
            both = one + other
            total[shell] = total[shell] + both if shell in total else both
            odd[member] = one - other
    density = sum(weight[shell] * total[shell] for shell in total)
    energy = sum(weight[SHELLS[v]] * v * total[SHELLS[v]] for v in (1.0, 3.0, 4.0, 8.0, 9.0))
    inverse = 1.0 / density
    drift = []
    for axis in range(3):
        parts = {}
        for member, value in odd.items():
            speed = SPEEDS[member][axis]
            if speed == 0:
                continue
            key = (SHELLS[square(member)], abs(speed))
            if key in parts:
                parts[key] = parts[key] + value if speed > 0 else parts[key] - value
            else:
                parts[key] = value if speed > 0 else -value
        flux = sum((weight[shell] * speed * 1.5) * value for (shell, speed), value in parts.items())
        drift.append(flux * inverse)
    w = drift
    ww = [value * value for value in w]
    norm = (ww[0] + ww[1] + ww[2]) * (4.0 / 9.0)
    t = (energy * inverse - norm) * 0.5 - 1.0
    b = 1.5 * norm
    scale = rate * density
    keep = 1.0 - rate
    tb = t * b
    t2 = t * t
    p0 = scale * (1.0 - 0.5 * b + 0.125 * b * b - 1.5 * t + 1.25 * tb + 1.875 * t2)
    p1 = scale * (0.5 * t - 0.25 * tb - 1.25 * t2)
    p2 = scale * (0.125 * t2)
    st = scale * t
    b0 = scale * (0.5 - 0.25 * b) - 1.75 * st
    c0 = scale * (1.0 - 0.5 * b) - 2.5 * st
    quart = {k: (k**4 / 24.0) * scale for k in (1, 2, 3)}
    cubic = {k: (k**3 / 6.0) * scale for k in (1, 2, 3)}
    reach = {"1": 1, "c": 1, "2": 2, "e": 2, "3": 3}
    coefficients = {}
    for value, shell in SHELLS.items():
        s = 1.5 * value
        even = p0 + s * p1 + (s * s) * p2 if s else p0
        if s:
            k = reach[shell]
            coefficients[shell] = (
                even,
                (k * k) * b0 + (k * k * s * 0.25) * st,
                k * c0 + (k * s * 0.5) * st,
                quart[k],
                cubic[k],
            )
        else:
            coefficients[shell] = even
    for member in range(Q):
        vector = SPEEDS[member]
        shell = SHELLS[square(member)]
        opposite = INDEX[tuple(-value for value in vector)]
        if member == opposite:
            store(member, keep * load(member) + coefficients[shell])
        elif member < opposite:
            k = reach[shell]
            q, q2 = None, None
            axes = [axis for axis in range(3) if vector[axis] != 0]
            if len(axes) == 1:
                q, q2 = w[axes[0]], ww[axes[0]]
            else:
                q = w[axes[0]]
                for axis in axes[1:]:
                    q = q + w[axis] if vector[axis] > 0 else q - w[axis]
                q2 = q * q
            e0, e2, o1, e4, o3 = coefficients[shell]
            even = e0 + q2 * (e2 + q2 * e4)
            uneven = q * (o1 + q2 * o3)
            store(member, keep * load(member) + (even + uneven))
            store(opposite, keep * load(opposite) + (even - uneven))


def exchange_kernel(
    sizes, g_hbm, r_hbm, p_ref, up_ref, down_ref,
    g, rate, zraw, zsend, zrecv, xzrecv, ysend, yrecv, yzrecv, dsend, drecv, dzrecv,
    load_sem, z_sem, xz_sem, y_sem, yz_sem, d_sem, dz_sem, x_sem, pair_sem, plane_sem, ready_sem,
):
    nx, ny, nz = sizes
    blocks = ny // 8
    signs = (1, -1)
    around = {}
    for axis in ("gx", "gy", "gz"):
        me, count = lax.axis_index(axis), lax.axis_size(axis)
        around[axis] = {1: lax.rem(me + 1, count), -1: lax.rem(me + count - 1, count)}

    def layer_load(x):
        return pltpu.make_async_copy(g_hbm.at[:, pl.ds(x, 1)], g.at[:, pl.ds(x, 1)], load_sem.at[x])

    rate_load = pltpu.make_async_copy(r_hbm, rate, load_sem.at[nx])
    rate_load.start()
    for x in [nx - 1, nx - 2, 0, 1] + list(range(2, nx - 2)):
        layer_load(x).start()

    barrier = pltpu.get_barrier_semaphore()
    gz = lax.axis_index("gz")
    core = lax.rem(gz, 2)
    chip = gz - core
    other_chip = lax.rem(chip + 2, lax.axis_size("gz"))
    partner = chip + 1 - core

    def tell(semaphore, **device):
        pl.semaphore_signal(semaphore, inc=1, device_id=device, device_id_type=MESH)

    for sign in signs:
        tell(barrier, gx=around["gx"][sign], gz=chip)
        tell(barrier, gy=around["gy"][sign], gz=chip + 1)
    tell(barrier, gz=other_chip)

    tell(barrier, gz=partner)

    lane = lax.broadcasted_iota(jnp.int32, (8, nz), 1)
    pack_masks = {offset: lane >= offset for offset in sorted(set(ZS[1].values())) if offset}

    def row_of(member, block):
        return pl.ds(final_row(member) + SPEEDS[member][1] + 8 * block, 8)

    def collide_block(x, block):
        pieces = {1: {}, -1: {}}

        def load(member):
            return g[member, x, pl.ds(8 * block, 8), :]

        def store(member, value):
            cz = SPEEDS[member][2]
            if cz != 0:
                p_ref[member, x, row_of(member, block), :] = pltpu.roll(value, cz % nz, 1)
                sign = 1 if cz > 0 else -1
                place = ZS[sign][member]
                shift = (place + max(cz, 0)) % nz
                pieces[sign][place] = pltpu.roll(value, shift, 1) if shift else value
            else:
                p_ref[member, x, row_of(member, block), :] = value

        collide(load, rate[x, pl.ds(8 * block, 8), :], store)
        for index, sign in enumerate(signs):
            packed = None
            for place in sorted(pieces[sign]):
                packed = pieces[sign][place] if packed is None else jnp.where(pack_masks[place], pieces[sign][place], packed)
            zraw[index, x, block] = packed

    def collide_layer(x, carry):
        layer_load(x).wait()
        for block in range(blocks):
            collide_block(x, block)
        return carry

    def column(half, block, offset):
        return 18 * (half * blocks + block) + offset

    def fold_z(index, pair):
        packed = None
        for half in range(2):
            for block in range(blocks):
                place = column(half, block, 0)
                value = zraw[index, 2 * pair + half, block]
                packed = value if packed is None else jnp.where(lane >= place, pltpu.roll(value, place, 1), packed)
        zsend[index, pair] = packed

    def enters(sign, reach):
        return lane < reach if sign > 0 else lane >= nz - reach

    def unfold(columns, target, member, half, block, rows):
        cz = SPEEDS[member][2]
        sign, reach = (1, cz) if cz > 0 else (-1, -cz)
        place = column(half, block, ZS[sign][member])
        shift = ((0 if sign > 0 else nz - reach) - place) % nz
        value = pltpu.roll(columns, shift, 1) if shift else columns
        pltpu.store(target.at[rows, :], value, mask=enters(sign, reach))

    def z_copy(index):
        return pltpu.make_async_remote_copy(
            zsend.at[index], zrecv.at[index], z_sem.at[0, index], z_sem.at[1, index],
            device_id={"gz": around["gz"][signs[index]]}, device_id_type=MESH,
        )

    def xz_copy(ix, iz):
        pair = nx // 2 - 1 if ix == 0 else 0
        return pltpu.make_async_remote_copy(
            zsend.at[iz, pair], xzrecv.at[ix, iz], xz_sem.at[0, ix, iz], xz_sem.at[1, ix, iz],
            device_id={"gx": around["gx"][signs[ix]], "gz": around["gz"][signs[iz]]}, device_id_type=MESH,
        )

    halo = (up_ref, down_ref)

    def x_copy(ix, member):
        sign, reach = signs[ix], abs(SPEEDS[member][0])
        rows = pl.ds(final_row(member), ny)
        layers = pl.ds(nx - reach, reach) if sign > 0 else pl.ds(0, reach)
        place = list(XS[sign]).index(member)
        return pltpu.make_async_remote_copy(
            p_ref.at[member, layers, rows, :], halo[ix].at[pl.ds(XS[sign][member], reach), rows, :],
            x_sem.at[0, ix, place], x_sem.at[1, ix, place],
            device_id={"gx": around["gx"][sign]}, device_id_type=MESH,
        )

    def d_copy(number):
        sx, sy = CORNERS[number]
        return pltpu.make_async_remote_copy(
            dsend.at[number], drecv.at[number], d_sem.at[0, number], d_sem.at[1, number],
            device_id={"gx": around["gx"][sx], "gy": around["gy"][sy]}, device_id_type=MESH,
        )

    def dz_copy(number, iz):
        sx, sy = CORNERS[number]
        return pltpu.make_async_remote_copy(
            dsend.at[number], dzrecv.at[number, iz], dz_sem.at[0, number, iz], dz_sem.at[1, number, iz],
            device_id={"gx": around["gx"][sx], "gy": around["gy"][sy], "gz": around["gz"][signs[iz]]},
            device_id_type=MESH,
        )

    def y_copy(iy):
        return pltpu.make_async_remote_copy(
            ysend.at[iy], yrecv.at[iy], y_sem.at[0, iy], y_sem.at[1, iy],
            device_id={"gy": around["gy"][signs[iy]]}, device_id_type=MESH,
        )

    def yz_copy(iy, iz):
        return pltpu.make_async_remote_copy(
            ysend.at[iy, pl.ds(18 - (2 - iz) * EDGE, EDGE)], yzrecv.at[iy, iz],
            yz_sem.at[0, iy, iz], yz_sem.at[1, iy, iz],
            device_id={"gy": around["gy"][signs[iy]], "gz": around["gz"][signs[iz]]}, device_id_type=MESH,
        )

    def slabs(fast):
        for members in (TILTED, FLAT):
            for ix, sign in enumerate(signs):
                for member in members[sign]:
                    if (abs(SPEEDS[member][0]) == 3) == fast:
                        x_copy(ix, member).start()

    def meet(own, count):
        @pl.when(core == own)
        def _():
            pl.semaphore_wait(barrier, count)
            tell(pair_sem, gz=partner)

        @pl.when(core != own)
        def _():
            pl.semaphore_wait(pair_sem, 1)

    def meet_x():
        meet(0, 7)

    def meet_y():
        meet(1, 5)

    def corners(iy):
        pl.semaphore_wait(ready_sem.at[iy], 1)
        for number, (sx, sy) in enumerate(CORNERS):
            if sy == signs[iy]:
                d_copy(number).start()
                for iz in range(2):
                    dz_copy(number, iz).start()

    def edges(iy):
        for iz in range(2):
            yz_copy(iy, iz).start()

    last = lax.axis_index("gy") == lax.axis_size("gy") - 1
    not_last = jnp.logical_not(last)
    first = lax.axis_index("gy") == 0
    x_first = lax.axis_index("gx") > 0
    rate_load.wait()
    lax.fori_loop(0, 2, lambda turn, carry: collide_layer(nx - 1 - turn, carry), 0)
    lax.fori_loop(0, 2, collide_layer, 0)
    for number, (sx, sy) in enumerate(CORNERS):
        for place, (member, layer, row) in enumerate(corner_rows(sx, sy)):
            x = nx - abs(SPEEDS[member][0]) + layer if sx > 0 else layer
            dsend[number, pl.ds(place, 1), :] = p_ref[member, x, pl.ds(leaving_row(member, row, ny), 1), :]

    def tell_plane():
        for sign in signs:
            tell(plane_sem, gz=around["gz"][sign])

    def tell_ready():
        pl.semaphore_wait(plane_sem, 2)
        for iy, sign in enumerate(signs):
            tell(ready_sem.at[1 - iy], gy=around["gy"][sign])

    x_last = jnp.logical_not(x_first)
    pl.when(last)(meet_y)

    @pl.when(x_first)
    def _():
        meet_x()
        tell_plane()

    @pl.when(last)
    def _():
        corners(0)

    @pl.when(x_first)
    def _():
        slabs(False)

    pl.when(jnp.logical_and(last, x_first))(tell_ready)
    lax.fori_loop(2, nx - 2, collide_layer, 0)

    @pl.when(x_first)
    def _():
        slabs(True)

    for iy, sign in enumerate(signs):
        for member, offset in YS[sign].items():
            for row in range(abs(SPEEDS[member][1])):
                ysend[iy, offset + row] = read_rows(p_ref, member, leaving_row(member, row, ny))

    pl.when(not_last)(meet_y)
    pl.when(jnp.logical_and(not_last, x_first))(tell_ready)
    for iy in range(2):
        y_copy(iy).start()

    @pl.when(last)
    def _():
        edges(0)

    @pl.when(x_last)
    def _():
        meet_x()
        tell_plane()

    for index in range(2):
        for pair in range(nx // 2):
            fold_z(index, pair)
    for index in range(2):
        z_copy(index).start()
    pl.when(x_last)(tell_ready)
    for ix in range(2):
        for iz in range(2):
            xz_copy(ix, iz).start()

    @pl.when(jnp.logical_not(x_first))
    def _():
        slabs(False)
        slabs(True)

    @pl.when(not_last)
    def _():
        corners(0)
        edges(0)

    def finish_edges():
        corners(1)
        edges(1)

    pl.when(jnp.logical_not(first))(finish_edges)

    def merge_z(index, wanted):
        for pair in range(nx // 2):
            columns = zrecv[index, pair]
            for half in range(2):
                for block in range(blocks):
                    for member in ZS[signs[index]]:
                        x = 2 * pair + half
                        if wanted(member, x):
                            unfold(columns, p_ref.at[member, x], member, half, block, row_of(member, block))

    def travels(member, x):
        cx = SPEEDS[member][0]
        return x >= nx - cx if cx > 0 else x < -cx

    for index in range(2):
        z_copy(index).wait_recv()
        merge_z(index, lambda member, x: not travels(member, x))
    pl.when(first)(finish_edges)
    for members in (TILTED, FLAT):
        for ix, sign in enumerate(signs):
            for member in members[sign]:
                x_copy(ix, member).wait_send()
    for index in range(2):
        merge_z(index, travels)
    for iy, sign in enumerate(signs):
        y_copy(iy).wait_recv()
        for iz in range(2):
            yz_copy(iy, iz).wait_recv()
        for member, offset in YS[sign].items():
            cz = SPEEDS[member][2]
            for row in range(abs(SPEEDS[member][1])):
                value = yrecv[iy, offset + row]
                if cz != 0:
                    iz = 0 if cz > 0 else 1
                    edge = yzrecv[iy, iz, offset + row - 18 + (2 - iz) * EDGE]
                    value = jnp.where(enters(signs[iz], abs(cz)), edge, value)
                write_rows(p_ref, member, entering_row(member, row, ny), value)
    for ix, sign in enumerate(signs):
        for iz in range(2):
            xz_copy(ix, iz).wait_recv()
        for member in TILTED[sign]:
            x_copy(ix, member).wait_recv()
            reach, iz = abs(SPEEDS[member][0]), 0 if SPEEDS[member][2] > 0 else 1
            for layer in range(reach):
                half = 2 - reach + layer if sign > 0 else layer
                for block in range(blocks):
                    target = halo[ix].at[XS[sign][member] + layer]
                    unfold(xzrecv[ix, iz], target, member, half, block, row_of(member, block))
    for ix, sign in enumerate(signs):
        for member in FLAT[sign]:
            x_copy(ix, member).wait_recv()
    for number, (sx, sy) in enumerate(CORNERS):
        ix = 0 if sx > 0 else 1
        d_copy(number).wait_recv()
        for iz in range(2):
            dz_copy(number, iz).wait_recv()
        for place, (member, layer, row) in enumerate(corner_rows(sx, sy)):
            cz = SPEEDS[member][2]
            value = drecv[number, pl.ds(place, 1), :]
            if cz != 0:
                iz = 0 if cz > 0 else 1
                mask = enters(signs[iz], abs(cz))[:1]
                value = jnp.where(mask, dzrecv[number, iz, pl.ds(place, 1), :], value)
            halo[ix][XS[sx][member] + layer, pl.ds(entering_row(member, row, ny), 1), :] = value
    for index in range(2):
        z_copy(index).wait_send()
        y_copy(index).wait_send()
        for iz in range(2):
            xz_copy(index, iz).wait_send()
            yz_copy(index, iz).wait_send()
    for number in range(4):
        d_copy(number).wait_send()
        for iz in range(2):
            dz_copy(number, iz).wait_send()


def emit_kernel(sizes, p_ref, up_ref, down_ref, o_hbm, sem):
    nx, ny, nz = sizes
    copies = []
    for member in range(Q):
        cx = SPEEDS[member][0]
        rows = pl.ds(final_row(member), ny)
        if cx > 0:
            pieces = [
                (p_ref.at[member, pl.ds(0, nx - cx), rows, :], o_hbm.at[member, pl.ds(cx, nx - cx)]),
                (up_ref.at[pl.ds(XS[1][member], cx), rows, :], o_hbm.at[member, pl.ds(0, cx)]),
            ]
        elif cx < 0:
            pieces = [
                (p_ref.at[member, pl.ds(-cx, nx + cx), rows, :], o_hbm.at[member, pl.ds(0, nx + cx)]),
                (down_ref.at[pl.ds(XS[-1][member], -cx), rows, :], o_hbm.at[member, pl.ds(nx + cx, -cx)]),
            ]
        else:
            pieces = [(p_ref.at[member, :, rows, :], o_hbm.at[member])]
        for source, target in pieces:
            copies.append(pltpu.make_async_copy(source, target, sem.at[len(copies)]))
    for copy in copies:
        copy.start()
    for copy in copies:
        copy.wait()


def per_device(populations, relax):
    sizes = populations.shape[1:]
    nx, ny, nz = sizes
    blocks = ny // 8
    vmem = pl.BlockSpec(memory_space=pltpu.VMEM)
    hbm = pl.BlockSpec(memory_space=pltpu.HBM)
    dma = pltpu.SemaphoreType.DMA
    shifted, up, down = pl.pallas_call(
        functools.partial(exchange_kernel, sizes),
        out_shape=(
            jax.ShapeDtypeStruct((Q, nx, ROWS, nz), F32),
            jax.ShapeDtypeStruct((18, ROWS, nz), F32),
            jax.ShapeDtypeStruct((18, ROWS, nz), F32),
        ),
        in_specs=[hbm, hbm],
        out_specs=(vmem, vmem, vmem),
        scratch_shapes=[
            pltpu.VMEM((Q, nx, ny, nz), F32),
            pltpu.VMEM((nx, ny, nz), F32),
            pltpu.VMEM((2, nx, blocks, 8, nz), F32),
            pltpu.VMEM((2, nx // 2, 8, nz), F32),
            pltpu.VMEM((2, nx // 2, 8, nz), F32),
            pltpu.VMEM((2, 2, 8, nz), F32),
            pltpu.VMEM((2, 18, nx, nz), F32),
            pltpu.VMEM((2, 18, nx, nz), F32),
            pltpu.VMEM((2, 2, EDGE, nx, nz), F32),
            pltpu.VMEM((4, 8, nz), F32),
            pltpu.VMEM((4, 8, nz), F32),
            pltpu.VMEM((4, 2, 8, nz), F32),
            dma((nx + 1,)),
            dma((2, 2)),
            dma((2, 2, 2)),
            dma((2, 2)),
            dma((2, 2, 2)),
            dma((2, 4)),
            dma((2, 4, 2)),
            dma((2, 2, 11)),
            pltpu.SemaphoreType.REGULAR,
            pltpu.SemaphoreType.REGULAR,
            pltpu.SemaphoreType.REGULAR((2,)),
        ],
        compiler_params=pltpu.CompilerParams(
            collective_id=0, has_side_effects=True, vmem_limit_bytes=24 * 1024 * 1024
        ),
        name="collide_exchange",
    )(*(pltpu.with_memory_space_constraint(array, pltpu.HBM) for array in (populations, relax)))
    return pl.pallas_call(
        functools.partial(emit_kernel, sizes),
        out_shape=jax.ShapeDtypeStruct(populations.shape, F32),
        in_specs=[vmem, vmem, vmem],
        out_specs=hbm,
        scratch_shapes=[dma((61,))],
        compiler_params=pltpu.CompilerParams(vmem_limit_bytes=24 * 1024 * 1024),
        name="emit",
    )(shifted, up, down)


def solution(mesh):
    return jax.shard_map(
        per_device,
        mesh=mesh,
        in_specs=(P(None, "gx", "gy", "gz"), P("gx", "gy", "gz")),
        out_specs=P(None, "gx", "gy", "gz"),
        check_vma=False,
    )
```

```python
import functools

import jax
import jax.numpy as jnp
from jax import lax
from jax.experimental import pallas as pl
from jax.experimental.pallas import tpu as pltpu
from jax.sharding import PartitionSpec as P

MESH = pl.DeviceIdType.MESH
F32 = jnp.float32


def lattice():
    speeds = [(0, 0, 0)]
    weights = [1.0 / 12.0]
    for axis in range(3):
        for sign in (1, -1):
            vector = [0, 0, 0]
            vector[axis] = sign
            speeds.append(tuple(vector))
            weights.append(1.0 / 12.0)
    for first in (1, -1):
        for second in (1, -1):
            for third in (1, -1):
                speeds.append((first, second, third))
                weights.append(1.0 / 27.0)
    for axis in range(3):
        for sign in (2, -2):
            vector = [0, 0, 0]
            vector[axis] = sign
            speeds.append(tuple(vector))
            weights.append(2.0 / 135.0)
    for couple in ((0, 1), (0, 2), (1, 2)):
        for first in (2, -2):
            for second in (2, -2):
                vector = [0, 0, 0]
                vector[couple[0]] = first
                vector[couple[1]] = second
                speeds.append(tuple(vector))
                weights.append(1.0 / 432.0)
    for axis in range(3):
        for sign in (3, -3):
            vector = [0, 0, 0]
            vector[axis] = sign
            speeds.append(tuple(vector))
            weights.append(1.0 / 1620.0)
    return speeds, weights


SPEEDS, WEIGHTS = lattice()
Q = 39
INDEX = {vector: member for member, vector in enumerate(SPEEDS)}
ROWS = 32


def slots(axis, sign):
    table, offset = {}, 0
    for third in (0, 1, -1):
        for member in range(Q):
            speed = SPEEDS[member][axis] * sign
            cz = SPEEDS[member][2] if axis < 2 else 0
            if speed > 0 and (cz > 0) - (cz < 0) == third:
                table[member] = offset
                offset += speed
    return table


XS = {sign: slots(0, sign) for sign in (1, -1)}
YS = {sign: slots(1, sign) for sign in (1, -1)}
ZS = {sign: slots(2, sign) for sign in (1, -1)}
FLAT = {sign: [m for m in XS[sign] if SPEEDS[m][2] == 0] for sign in (1, -1)}
TILTED = {sign: [m for m in XS[sign] if SPEEDS[m][2] != 0] for sign in (1, -1)}
EDGE = 4
CORNERS = [(1, 1), (1, -1), (-1, 1), (-1, -1)]
SHELLS = {0.0: "0", 1.0: "1", 3.0: "c", 4.0: "2", 8.0: "e", 9.0: "3"}


def square(member):
    return float(sum(value * value for value in SPEEDS[member]))


def final_row(member):
    return 8 if SPEEDS[member][1] < 0 else 0


def corner_rows(sx, sy):
    rows = []
    for member in range(Q):
        cx, cy = SPEEDS[member][0] * sx, SPEEDS[member][1] * sy
        if cx > 0 and cy > 0:
            rows += [(member, layer, row) for layer in range(cx) for row in range(cy)]
    return rows


def leaving_row(member, row, ny):
    cy = SPEEDS[member][1]
    return ny + row if cy > 0 else 8 + cy + row


def entering_row(member, row, ny):
    cy = SPEEDS[member][1]
    return row if cy > 0 else 8 + ny + cy + row


def strided(ref, member, row):
    count, layers, rows, lanes = ref.shape
    return ref.reshape(count * layers * rows, lanes), pl.ds(member * layers * rows + row, layers, stride=rows)


def read_rows(ref, member, row):
    flat, where = strided(ref, member, row)
    return flat[where, :]


def write_rows(ref, member, row, value):
    flat, where = strided(ref, member, row)
    flat[where, :] = value


def collide(load, rate, store):
    weight = {shell: WEIGHTS[m] for m in range(Q) for shell in [SHELLS[square(m)]]}
    total = {}
    odd = {}
    for member in range(Q):
        vector = SPEEDS[member]
        shell = SHELLS[square(member)]
        opposite = INDEX[tuple(-value for value in vector)]
        if member == opposite:
            total[shell] = load(member)
        elif member < opposite:
            one, other = load(member), load(opposite)
            both = one + other
            total[shell] = total[shell] + both if shell in total else both
            odd[member] = one - other
    density = sum(weight[shell] * total[shell] for shell in total)
    energy = sum(weight[SHELLS[v]] * v * total[SHELLS[v]] for v in (1.0, 3.0, 4.0, 8.0, 9.0))
    inverse = 1.0 / density
    drift = []
    for axis in range(3):
        parts = {}
        for member, value in odd.items():
            speed = SPEEDS[member][axis]
            if speed == 0:
                continue
            key = (SHELLS[square(member)], abs(speed))
            if key in parts:
                parts[key] = parts[key] + value if speed > 0 else parts[key] - value
            else:
                parts[key] = value if speed > 0 else -value
        flux = sum((weight[shell] * speed * 1.5) * value for (shell, speed), value in parts.items())
        drift.append(flux * inverse)
    w = drift
    ww = [value * value for value in w]
    norm = (ww[0] + ww[1] + ww[2]) * (4.0 / 9.0)
    t = (energy * inverse - norm) * 0.5 - 1.0
    b = 1.5 * norm
    scale = rate * density
    keep = 1.0 - rate
    tb = t * b
    t2 = t * t
    p0 = scale * (1.0 - 0.5 * b + 0.125 * b * b - 1.5 * t + 1.25 * tb + 1.875 * t2)
    p1 = scale * (0.5 * t - 0.25 * tb - 1.25 * t2)
    p2 = scale * (0.125 * t2)
    st = scale * t
    b0 = scale * (0.5 - 0.25 * b) - 1.75 * st
    c0 = scale * (1.0 - 0.5 * b) - 2.5 * st
    quart = {k: (k**4 / 24.0) * scale for k in (1, 2, 3)}
    cubic = {k: (k**3 / 6.0) * scale for k in (1, 2, 3)}
    reach = {"1": 1, "c": 1, "2": 2, "e": 2, "3": 3}
    coefficients = {}
    for value, shell in SHELLS.items():
        s = 1.5 * value
        even = p0 + s * p1 + (s * s) * p2 if s else p0
        if s:
            k = reach[shell]
            coefficients[shell] = (
                even,
                (k * k) * b0 + (k * k * s * 0.25) * st,
                k * c0 + (k * s * 0.5) * st,
                quart[k],
                cubic[k],
            )
        else:
            coefficients[shell] = even
    for member in range(Q):
        vector = SPEEDS[member]
        shell = SHELLS[square(member)]
        opposite = INDEX[tuple(-value for value in vector)]
        if member == opposite:
            store(member, keep * load(member) + coefficients[shell])
        elif member < opposite:
            k = reach[shell]
            q, q2 = None, None
            axes = [axis for axis in range(3) if vector[axis] != 0]
            if len(axes) == 1:
                q, q2 = w[axes[0]], ww[axes[0]]
            else:
                q = w[axes[0]]
                for axis in axes[1:]:
                    q = q + w[axis] if vector[axis] > 0 else q - w[axis]
                q2 = q * q
            e0, e2, o1, e4, o3 = coefficients[shell]
            even = e0 + q2 * (e2 + q2 * e4)
            uneven = q * (o1 + q2 * o3)
            store(member, keep * load(member) + (even + uneven))
            store(opposite, keep * load(opposite) + (even - uneven))


def exchange_kernel(
    sizes, g_hbm, r_hbm, p_ref, up_ref, down_ref,
    g, rate, zraw, zsend, zrecv, xzrecv, ysend, yrecv, yzrecv, dsend, drecv, dzrecv,
    load_sem, z_sem, xz_sem, y_sem, yz_sem, d_sem, dz_sem, x_sem, pair_sem, plane_sem, ready_sem,
):
    nx, ny, nz = sizes
    blocks = ny // 8
    signs = (1, -1)
    around = {}
    for axis in ("gx", "gy", "gz"):
        me, count = lax.axis_index(axis), lax.axis_size(axis)
        around[axis] = {1: lax.rem(me + 1, count), -1: lax.rem(me + count - 1, count)}

    def layer_load(x):
        return pltpu.make_async_copy(g_hbm.at[:, pl.ds(x, 1)], g.at[:, pl.ds(x, 1)], load_sem.at[x])

    rate_load = pltpu.make_async_copy(r_hbm, rate, load_sem.at[nx])
    rate_load.start()
    for x in [nx - 1, nx - 2, 0, 1] + list(range(2, nx - 2)):
        layer_load(x).start()

    barrier = pltpu.get_barrier_semaphore()
    gz = lax.axis_index("gz")
    core = lax.rem(gz, 2)
    chip = gz - core
    other_chip = lax.rem(chip + 2, lax.axis_size("gz"))
    partner = chip + 1 - core

    def tell(semaphore, **device):
        pl.semaphore_signal(semaphore, inc=1, device_id=device, device_id_type=MESH)

    for sign in signs:
        tell(barrier, gx=around["gx"][sign], gz=chip)
        tell(barrier, gy=around["gy"][sign], gz=chip + 1)
    tell(barrier, gz=other_chip)

    tell(barrier, gz=partner)

    lane = lax.broadcasted_iota(jnp.int32, (8, nz), 1)
    pack_masks = {offset: lane >= offset for offset in sorted(set(ZS[1].values())) if offset}

    def row_of(member, block):
        return pl.ds(final_row(member) + SPEEDS[member][1] + 8 * block, 8)

    def collide_block(x, block):
        pieces = {1: {}, -1: {}}

        def load(member):
            return g[member, x, pl.ds(8 * block, 8), :]

        def store(member, value):
            cz = SPEEDS[member][2]
            if cz != 0:
                p_ref[member, x, row_of(member, block), :] = pltpu.roll(value, cz % nz, 1)
                sign = 1 if cz > 0 else -1
                place = ZS[sign][member]
                shift = (place + max(cz, 0)) % nz
                pieces[sign][place] = pltpu.roll(value, shift, 1) if shift else value
            else:
                p_ref[member, x, row_of(member, block), :] = value

        collide(load, rate[x, pl.ds(8 * block, 8), :], store)
        for index, sign in enumerate(signs):
            packed = None
            for place in sorted(pieces[sign]):
                packed = pieces[sign][place] if packed is None else jnp.where(pack_masks[place], pieces[sign][place], packed)
            zraw[index, x, block] = packed

    def collide_layer(x, carry):
        layer_load(x).wait()
        for block in range(blocks):
            collide_block(x, block)
        return carry

    def column(half, block, offset):
        return 18 * (half * blocks + block) + offset

    def fold_z(index, pair):
        packed = None
        for half in range(2):
            for block in range(blocks):
                place = column(half, block, 0)
                value = zraw[index, 2 * pair + half, block]
                packed = value if packed is None else jnp.where(lane >= place, pltpu.roll(value, place, 1), packed)
        zsend[index, pair] = packed

    def enters(sign, reach):
        return lane < reach if sign > 0 else lane >= nz - reach

    def unfold(columns, target, member, half, block, rows):
        cz = SPEEDS[member][2]
        sign, reach = (1, cz) if cz > 0 else (-1, -cz)
        place = column(half, block, ZS[sign][member])
        shift = ((0 if sign > 0 else nz - reach) - place) % nz
        value = pltpu.roll(columns, shift, 1) if shift else columns
        pltpu.store(target.at[rows, :], value, mask=enters(sign, reach))

    def z_copy(index):
        return pltpu.make_async_remote_copy(
            zsend.at[index], zrecv.at[index], z_sem.at[0, index], z_sem.at[1, index],
            device_id={"gz": around["gz"][signs[index]]}, device_id_type=MESH,
        )

    def xz_copy(ix, iz):
        pair = nx // 2 - 1 if ix == 0 else 0
        return pltpu.make_async_remote_copy(
            zsend.at[iz, pair], xzrecv.at[ix, iz], xz_sem.at[0, ix, iz], xz_sem.at[1, ix, iz],
            device_id={"gx": around["gx"][signs[ix]], "gz": around["gz"][signs[iz]]}, device_id_type=MESH,
        )

    halo = (up_ref, down_ref)

    def x_copy(ix, member):
        sign, reach = signs[ix], abs(SPEEDS[member][0])
        rows = pl.ds(final_row(member), ny)
        layers = pl.ds(nx - reach, reach) if sign > 0 else pl.ds(0, reach)
        place = group_of(member)
        return pltpu.make_async_remote_copy(
            p_ref.at[member, layers, rows, :], halo[ix].at[pl.ds(XS[sign][member], reach), rows, :],
            x_sem.at[0, ix, place], x_sem.at[1, ix, place],
            device_id={"gx": around["gx"][sign]}, device_id_type=MESH,
        )

    def group_of(member):
        return 0 if SPEEDS[member][2] != 0 else 1 if abs(SPEEDS[member][0]) < 3 else 2

    def x_group(ix, group):
        members = [m for m in XS[signs[ix]] if group_of(m) == group]
        count = sum(abs(SPEEDS[m][0]) for m in members)
        layers = halo[ix].at[pl.ds(XS[signs[ix]][members[0]], count), pl.ds(0, ny), :]
        return pltpu.make_async_remote_copy(
            layers, layers, x_sem.at[0, ix, group], x_sem.at[1, ix, group],
            device_id={"gx": around["gx"][signs[ix]]}, device_id_type=MESH,
        )

    def d_copy(number):
        sx, sy = CORNERS[number]
        return pltpu.make_async_remote_copy(
            dsend.at[number], drecv.at[number], d_sem.at[0, number], d_sem.at[1, number],
            device_id={"gx": around["gx"][sx], "gy": around["gy"][sy]}, device_id_type=MESH,
        )

    def dz_copy(number, iz):
        sx, sy = CORNERS[number]
        return pltpu.make_async_remote_copy(
            dsend.at[number], dzrecv.at[number, iz], dz_sem.at[0, number, iz], dz_sem.at[1, number, iz],
            device_id={"gx": around["gx"][sx], "gy": around["gy"][sy], "gz": around["gz"][signs[iz]]},
            device_id_type=MESH,
        )

    def y_copy(iy):
        return pltpu.make_async_remote_copy(
            ysend.at[iy], yrecv.at[iy], y_sem.at[0, iy], y_sem.at[1, iy],
            device_id={"gy": around["gy"][signs[iy]]}, device_id_type=MESH,
        )

    def yz_copy(iy, iz):
        return pltpu.make_async_remote_copy(
            ysend.at[iy, pl.ds(18 - (2 - iz) * EDGE, EDGE)], yzrecv.at[iy, iz],
            yz_sem.at[0, iy, iz], yz_sem.at[1, iy, iz],
            device_id={"gy": around["gy"][signs[iy]], "gz": around["gz"][signs[iz]]}, device_id_type=MESH,
        )

    def slabs(fast):
        for members in (TILTED, FLAT):
            for ix, sign in enumerate(signs):
                for member in members[sign]:
                    if (abs(SPEEDS[member][0]) == 3) == fast:
                        x_copy(ix, member).start()

    def meet(own, count):
        @pl.when(core == own)
        def _():
            pl.semaphore_wait(barrier, count)
            tell(pair_sem, gz=partner)

        @pl.when(core != own)
        def _():
            pl.semaphore_wait(pair_sem, 1)

    def meet_x():
        meet(0, 7)

    def meet_y():
        meet(1, 5)

    def corners(iy):
        pl.semaphore_wait(ready_sem.at[iy], 1)
        for number, (sx, sy) in enumerate(CORNERS):
            if sy == signs[iy]:
                d_copy(number).start()
                for iz in range(2):
                    dz_copy(number, iz).start()

    def edges(iy):
        for iz in range(2):
            yz_copy(iy, iz).start()

    last = lax.axis_index("gy") == lax.axis_size("gy") - 1
    not_last = jnp.logical_not(last)
    first = lax.axis_index("gy") == 0
    x_first = lax.axis_index("gx") > 0
    rate_load.wait()
    lax.fori_loop(0, 2, lambda turn, carry: collide_layer(nx - 1 - turn, carry), 0)
    lax.fori_loop(0, 2, collide_layer, 0)
    for number, (sx, sy) in enumerate(CORNERS):
        for place, (member, layer, row) in enumerate(corner_rows(sx, sy)):
            x = nx - abs(SPEEDS[member][0]) + layer if sx > 0 else layer
            dsend[number, pl.ds(place, 1), :] = p_ref[member, x, pl.ds(leaving_row(member, row, ny), 1), :]

    def tell_plane():
        for sign in signs:
            tell(plane_sem, gz=around["gz"][sign])

    def tell_ready():
        pl.semaphore_wait(plane_sem, 2)
        for iy, sign in enumerate(signs):
            tell(ready_sem.at[1 - iy], gy=around["gy"][sign])

    x_last = jnp.logical_not(x_first)
    pl.when(last)(meet_y)

    @pl.when(x_first)
    def _():
        meet_x()
        tell_plane()

    @pl.when(last)
    def _():
        corners(0)

    @pl.when(x_first)
    def _():
        slabs(False)

    pl.when(jnp.logical_and(last, x_first))(tell_ready)
    lax.fori_loop(2, nx - 2, collide_layer, 0)

    @pl.when(x_first)
    def _():
        slabs(True)

    for iy, sign in enumerate(signs):
        for member, offset in YS[sign].items():
            for row in range(abs(SPEEDS[member][1])):
                ysend[iy, offset + row] = read_rows(p_ref, member, leaving_row(member, row, ny))

    for index in range(2):
        for pair in range(nx // 2):
            fold_z(index, pair)

    def send_z():
        for index in range(2):
            z_copy(index).start()

    pl.when(x_first)(send_z)
    pl.when(not_last)(meet_y)
    pl.when(jnp.logical_and(not_last, x_first))(tell_ready)
    for iy in range(2):
        y_copy(iy).start()

    @pl.when(last)
    def _():
        edges(0)

    @pl.when(x_last)
    def _():
        meet_x()
        tell_plane()

    pl.when(x_last)(send_z)
    pl.when(x_last)(tell_ready)
    for ix in range(2):
        for iz in range(2):
            xz_copy(ix, iz).start()

    @pl.when(jnp.logical_not(x_first))
    def _():
        slabs(False)
        slabs(True)

    @pl.when(not_last)
    def _():
        corners(0)
        edges(0)

    def finish_edges():
        corners(1)
        edges(1)

    pl.when(jnp.logical_not(first))(finish_edges)

    def merge_z(index, wanted):
        for pair in range(nx // 2):
            columns = zrecv[index, pair]
            for half in range(2):
                for block in range(blocks):
                    for member in ZS[signs[index]]:
                        x = 2 * pair + half
                        if wanted(member, x):
                            unfold(columns, p_ref.at[member, x], member, half, block, row_of(member, block))

    def travels(member, x):
        cx = SPEEDS[member][0]
        return x >= nx - cx if cx > 0 else x < -cx

    for index in range(2):
        z_copy(index).wait_recv()
        merge_z(index, lambda member, x: not travels(member, x))
    pl.when(first)(finish_edges)
    for group in range(3):
        for ix in range(2):
            x_group(ix, group).wait_send()
    for index in range(2):
        merge_z(index, travels)
    for iy, sign in enumerate(signs):
        y_copy(iy).wait_recv()
        for iz in range(2):
            yz_copy(iy, iz).wait_recv()
        for member, offset in YS[sign].items():
            cz = SPEEDS[member][2]
            for row in range(abs(SPEEDS[member][1])):
                value = yrecv[iy, offset + row]
                if cz != 0:
                    iz = 0 if cz > 0 else 1
                    edge = yzrecv[iy, iz, offset + row - 18 + (2 - iz) * EDGE]
                    value = jnp.where(enters(signs[iz], abs(cz)), edge, value)
                write_rows(p_ref, member, entering_row(member, row, ny), value)
    for ix, sign in enumerate(signs):
        for iz in range(2):
            xz_copy(ix, iz).wait_recv()
        x_group(ix, 0).wait_recv()
        for member in TILTED[sign]:
            reach, iz = abs(SPEEDS[member][0]), 0 if SPEEDS[member][2] > 0 else 1
            for layer in range(reach):
                half = 2 - reach + layer if sign > 0 else layer
                for block in range(blocks):
                    target = halo[ix].at[XS[sign][member] + layer]
                    unfold(xzrecv[ix, iz], target, member, half, block, row_of(member, block))
    for ix in range(2):
        for group in (1, 2):
            x_group(ix, group).wait_recv()
    for number, (sx, sy) in enumerate(CORNERS):
        ix = 0 if sx > 0 else 1
        d_copy(number).wait_recv()
        for iz in range(2):
            dz_copy(number, iz).wait_recv()
        for place, (member, layer, row) in enumerate(corner_rows(sx, sy)):
            cz = SPEEDS[member][2]
            value = drecv[number, pl.ds(place, 1), :]
            if cz != 0:
                iz = 0 if cz > 0 else 1
                mask = enters(signs[iz], abs(cz))[:1]
                value = jnp.where(mask, dzrecv[number, iz, pl.ds(place, 1), :], value)
            halo[ix][XS[sx][member] + layer, pl.ds(entering_row(member, row, ny), 1), :] = value
    for index in range(2):
        z_copy(index).wait_send()
        y_copy(index).wait_send()
        for iz in range(2):
            xz_copy(index, iz).wait_send()
            yz_copy(index, iz).wait_send()
    for number in range(4):
        d_copy(number).wait_send()
        for iz in range(2):
            dz_copy(number, iz).wait_send()


def emit_kernel(sizes, p_ref, up_ref, down_ref, o_hbm, sem):
    nx, ny, nz = sizes
    copies = []
    for member in range(Q):
        cx = SPEEDS[member][0]
        rows = pl.ds(final_row(member), ny)
        if cx > 0:
            pieces = [
                (p_ref.at[member, pl.ds(0, nx - cx), rows, :], o_hbm.at[member, pl.ds(cx, nx - cx)]),
                (up_ref.at[pl.ds(XS[1][member], cx), rows, :], o_hbm.at[member, pl.ds(0, cx)]),
            ]
        elif cx < 0:
            pieces = [
                (p_ref.at[member, pl.ds(-cx, nx + cx), rows, :], o_hbm.at[member, pl.ds(0, nx + cx)]),
                (down_ref.at[pl.ds(XS[-1][member], -cx), rows, :], o_hbm.at[member, pl.ds(nx + cx, -cx)]),
            ]
        else:
            pieces = [(p_ref.at[member, :, rows, :], o_hbm.at[member])]
        for source, target in pieces:
            copies.append(pltpu.make_async_copy(source, target, sem.at[len(copies)]))
    for copy in copies:
        copy.start()
    for copy in copies:
        copy.wait()


def per_device(populations, relax):
    sizes = populations.shape[1:]
    nx, ny, nz = sizes
    blocks = ny // 8
    vmem = pl.BlockSpec(memory_space=pltpu.VMEM)
    hbm = pl.BlockSpec(memory_space=pltpu.HBM)
    dma = pltpu.SemaphoreType.DMA
    shifted, up, down = pl.pallas_call(
        functools.partial(exchange_kernel, sizes),
        out_shape=(
            jax.ShapeDtypeStruct((Q, nx, ROWS, nz), F32),
            jax.ShapeDtypeStruct((18, ROWS, nz), F32),
            jax.ShapeDtypeStruct((18, ROWS, nz), F32),
        ),
        in_specs=[hbm, hbm],
        out_specs=(vmem, vmem, vmem),
        scratch_shapes=[
            pltpu.VMEM((Q, nx, ny, nz), F32),
            pltpu.VMEM((nx, ny, nz), F32),
            pltpu.VMEM((2, nx, blocks, 8, nz), F32),
            pltpu.VMEM((2, nx // 2, 8, nz), F32),
            pltpu.VMEM((2, nx // 2, 8, nz), F32),
            pltpu.VMEM((2, 2, 8, nz), F32),
            pltpu.VMEM((2, 18, nx, nz), F32),
            pltpu.VMEM((2, 18, nx, nz), F32),
            pltpu.VMEM((2, 2, EDGE, nx, nz), F32),
            pltpu.VMEM((4, 8, nz), F32),
            pltpu.VMEM((4, 8, nz), F32),
            pltpu.VMEM((4, 2, 8, nz), F32),
            dma((nx + 1,)),
            dma((2, 2)),
            dma((2, 2, 2)),
            dma((2, 2)),
            dma((2, 2, 2)),
            dma((2, 4)),
            dma((2, 4, 2)),
            dma((2, 2, 3)),
            pltpu.SemaphoreType.REGULAR,
            pltpu.SemaphoreType.REGULAR,
            pltpu.SemaphoreType.REGULAR((2,)),
        ],
        compiler_params=pltpu.CompilerParams(
            collective_id=0, has_side_effects=True, vmem_limit_bytes=24 * 1024 * 1024
        ),
        name="collide_exchange",
    )(*(pltpu.with_memory_space_constraint(array, pltpu.HBM) for array in (populations, relax)))
    return pl.pallas_call(
        functools.partial(emit_kernel, sizes),
        out_shape=jax.ShapeDtypeStruct(populations.shape, F32),
        in_specs=[vmem, vmem, vmem],
        out_specs=hbm,
        scratch_shapes=[dma((61,))],
        compiler_params=pltpu.CompilerParams(vmem_limit_bytes=24 * 1024 * 1024),
        name="emit",
    )(shifted, up, down)


def solution(mesh):
    return jax.shard_map(
        per_device,
        mesh=mesh,
        in_specs=(P(None, "gx", "gy", "gz"), P("gx", "gy", "gz")),
        out_specs=P(None, "gx", "gy", "gz"),
        check_vma=False,
    )
```
